128 devices in a mesh: dp: 1, model: 2 (over core), ctx: 64 (over z, y, x).
Axes of the slice: x: 4, y: 4, z: 4, core: 2. Of those that a mesh axis runs over, the one named last changes fastest.
Arguments:
- x_tokens: bfloat16 [4096, 7168], P(('dp', 'ctx'))
- positions: int32 [4096], P(('dp', 'ctx'))
- w_dq: bfloat16 [7168, 1536], replicated
- gain_q: float32 [1536], replicated
- w_uq: bfloat16 [1536, 8192], P(None, 'model')
- w_qr: bfloat16 [1536, 4096], P(None, 'model')
- w_dkv: bfloat16 [7168, 512], replicated
- gain_kv: float32 [512], replicated
- w_kr: bfloat16 [7168, 64], replicated
- w_uk: bfloat16 [512, 8192], P(None, 'model')
- w_uv: bfloat16 [512, 8192], P(None, 'model')
- w_out: bfloat16 [8192, 7168], P('model')
Outputs:
- output: bfloat16 [4096, 7168], P(('dp', 'ctx', 'model'))
All inputs are finite; a program needn't handle non-finite values.
Results may differ from the reference program's by a relative error of at most 0.00810006.
Values are sent between devices in bfloat16 or wider.
A program may use at most 1 GiB of HBM per device.

```python
import jax
import jax.numpy as jnp
from jax import lax

HIDDEN = 7168
NUM_HEADS = 64
Q_RANK = 1536
KV_RANK = 512
NOPE_DIM = 128
ROPE_DIM = 64
V_DIM = 128
TOKENS_DEV = 64
CTX_DEVS = 64
SEQ_LEN = 4096

SPAN_LEN = TOKENS_DEV // 2
QUERY_BLOCK = min(TOKENS_DEV, 256)
NORM_EPS = 1e-6
ROPE_BASE = 10000.0


def rms_norm(hidden, gain):
    mean_sq = jnp.mean(hidden * hidden, axis=-1, keepdims=True)
    return (hidden * lax.rsqrt(mean_sq + NORM_EPS) * gain).astype(jnp.bfloat16)


def apply_rope(vals, positions):
    half_dim = vals.shape[-1] // 2
    inv_freq = ROPE_BASE ** (-(jnp.arange(half_dim, dtype=jnp.float32) * 2.0 / vals.shape[-1]))
    angles = positions.astype(jnp.float32)[:, None] * inv_freq[None, :]
    angles = angles.reshape((vals.shape[0],) + (1,) * (vals.ndim - 2) + (half_dim,))
    cos_ang = jnp.cos(angles)
    sin_ang = jnp.sin(angles)
    lower_half = vals[..., :half_dim]
    upper_half = vals[..., half_dim:]
    return jnp.concatenate([lower_half * cos_ang - upper_half * sin_ang, upper_half * cos_ang + lower_half * sin_ang], axis=-1)


def draw_positions(rng_key):
    steps = jax.random.randint(rng_key, (SEQ_LEN,), 1, 3, dtype=jnp.int32)
    logical = (jnp.cumsum(steps) - steps[0]).astype(jnp.int32)
    device_idx = jnp.arange(CTX_DEVS)[:, None, None]
    half_idx = jnp.arange(2)[None, :, None]
    offset = jnp.arange(SPAN_LEN)[None, None, :]
    span_id = jnp.where(half_idx == 0, device_idx, 2 * CTX_DEVS - 1 - device_idx)
    storage_idx = (span_id * SPAN_LEN + offset).reshape(SEQ_LEN)
    return logical[storage_idx]


def setup_inputs(seed: int = 0, part: int = 0) -> dict:
    base_key = jax.random.key(seed)
    part_key = jax.random.fold_in(base_key, part)
    key_x, key_pos = jax.random.split(part_key)
    weight_keys = jax.random.split(jax.random.key(seed + 1), 10)

    def weight(rng_key, arr_shape, fan_in, scale_gain):
        return (jax.random.normal(rng_key, arr_shape, jnp.float32) * (scale_gain * fan_in ** -0.5)).astype(jnp.bfloat16)

    return {
        'x_tokens': jax.random.normal(key_x, (SEQ_LEN, HIDDEN), jnp.float32).astype(jnp.bfloat16),
        'positions': draw_positions(key_pos),
        'w_dq': weight(weight_keys[0], (HIDDEN, Q_RANK), HIDDEN, 1.0),
        'gain_q': 1.0 + 0.25 * jax.random.normal(weight_keys[1], (Q_RANK,), jnp.float32),
        'w_uq': weight(weight_keys[2], (Q_RANK, NUM_HEADS * NOPE_DIM), Q_RANK, 1.5),
        'w_qr': weight(weight_keys[3], (Q_RANK, NUM_HEADS * ROPE_DIM), Q_RANK, 1.5),
        'w_dkv': weight(weight_keys[4], (HIDDEN, KV_RANK), HIDDEN, 1.0),
        'gain_kv': 1.0 + 0.25 * jax.random.normal(weight_keys[5], (KV_RANK,), jnp.float32),
        'w_kr': weight(weight_keys[6], (HIDDEN, ROPE_DIM), HIDDEN, 1.0),
        'w_uk': weight(weight_keys[7], (KV_RANK, NUM_HEADS * NOPE_DIM), KV_RANK, 1.0),
        'w_uv': weight(weight_keys[8], (KV_RANK, NUM_HEADS * V_DIM), KV_RANK, 1.0),
        'w_out': weight(weight_keys[9], (NUM_HEADS * V_DIM, HIDDEN), NUM_HEADS * V_DIM, 1.0),
    }


def reference(x_tokens, positions, w_dq, gain_q, w_uq, w_qr, w_dkv, gain_kv, w_kr, w_uk, w_uv, w_out):
    c_q = rms_norm(jnp.dot(x_tokens, w_dq, preferred_element_type=jnp.float32), gain_q)
    c_kv = rms_norm(jnp.dot(x_tokens, w_dkv, preferred_element_type=jnp.float32), gain_kv)
    k_rope = apply_rope(jnp.dot(x_tokens, w_kr, preferred_element_type=jnp.float32), positions).astype(jnp.bfloat16)
    per_head = (
        w_uq.reshape(Q_RANK, NUM_HEADS, NOPE_DIM).transpose(1, 0, 2),
        w_qr.reshape(Q_RANK, NUM_HEADS, ROPE_DIM).transpose(1, 0, 2),
        w_uk.reshape(KV_RANK, NUM_HEADS, NOPE_DIM).transpose(1, 0, 2),
        w_uv.reshape(KV_RANK, NUM_HEADS, V_DIM).transpose(1, 0, 2),
        w_out.reshape(NUM_HEADS, V_DIM, HIDDEN),
    )
    score_scale = (NOPE_DIM + ROPE_DIM) ** -0.5
    num_blocks = SEQ_LEN // QUERY_BLOCK
    query_pos = positions.reshape(num_blocks, QUERY_BLOCK)

    def head_step(y_acc, head_w):
        w_uq_h, w_qr_h, w_uk_h, w_uv_h, w_out_h = head_w
        q_nope = jnp.dot(c_q, w_uq_h, preferred_element_type=jnp.float32).astype(jnp.bfloat16)
        q_rope = apply_rope(jnp.dot(c_q, w_qr_h, preferred_element_type=jnp.float32), positions).astype(jnp.bfloat16)
        k_nope = jnp.dot(c_kv, w_uk_h, preferred_element_type=jnp.float32).astype(jnp.bfloat16)
        v_full = jnp.dot(c_kv, w_uv_h, preferred_element_type=jnp.float32).astype(jnp.bfloat16).astype(jnp.float32)

        def query_block(blk_in):
            qn_blk, qr_blk, qpos_blk = blk_in
            scores = (jnp.dot(qn_blk, k_nope.T, preferred_element_type=jnp.float32) + jnp.dot(qr_blk, k_rope.T, preferred_element_type=jnp.float32)) * score_scale
            allowed = positions[None, :] <= qpos_blk[:, None]
            weights = jax.nn.softmax(jnp.where(allowed, scores, -jnp.inf), axis=-1)
            return jnp.dot(weights, v_full).astype(jnp.bfloat16)

        out_head = lax.map(query_block, (q_nope.reshape(num_blocks, QUERY_BLOCK, NOPE_DIM), q_rope.reshape(num_blocks, QUERY_BLOCK, ROPE_DIM), query_pos)).reshape(SEQ_LEN, V_DIM)
        return y_acc + jnp.dot(out_head, w_out_h, preferred_element_type=jnp.float32), None

    y_acc = lax.scan(head_step, jnp.zeros((SEQ_LEN, HIDDEN), jnp.float32), per_head)[0]
    return y_acc.astype(jnp.bfloat16)
```

```python
import math

import numpy as np
import jax
import jax.numpy as jnp
from jax import lax
from jax.experimental import pallas as pl
from jax.experimental.pallas import tpu as pltpu
from jax.sharding import PartitionSpec as P

NORM_EPS = 1e-6
ROPE_BASE = 10000.0
NEG_BIG = -1e30
MESH = pl.DeviceIdType.MESH
BF = jnp.bfloat16
F32 = jnp.float32

HIDDEN = 7168
Q_RANK = 1536
KV_RANK = 512
TOK = 64
SPAN = 32
HALF_SPAN = SPAN // 2
LANES = 128
QH = Q_RANK // 2
KH = KV_RANK // 2
BLK = 512
QB = 256
QK_DIM = 192
KEYS = 4096
ROWS_H = KEYS // 2
N_DOWN = HIDDEN // BLK
N_SIDE = N_DOWN // 2
N_OUT = HIDDEN // BLK
N_SLOTS = 8
N_EARLY = 4
N_TILES = 9
GROUP = 8
EXP_SCALE = QK_DIM ** -0.5 * math.log2(math.e)
LIMIT = 66 * 10 ** 6


def dot(a, b):
    return jnp.dot(a, b, preferred_element_type=F32)


def dot_dims(a, b, ca, cb):
    return lax.dot_general(a, b, (((ca,), (cb,)), ((), ())), preferred_element_type=F32)


def iota(shape, axis):
    return lax.broadcasted_iota(jnp.int32, shape, axis)


def dyn(i, width):
    return pl.ds(pl.multiple_of(i * width, math.gcd(width, BLK)), width)


class Ring:
    def __init__(self, blk, aux, p, right, left, ssem, rsem, row):
        prev, nxt, opp = (p + 3) % 4, (p + 1) % 4, (p + 2) % 4
        self.ssem, self.rsem, self.row = ssem, rsem, row
        self.sent = (
            (blk(p, 0), right, blk(prev, 0)),
            (blk(p, 1), left, blk(nxt, 1)),
            (aux(p), right, aux(prev)),
            (blk(p, 1), right, blk(prev, 1)),
            (blk(p, 0), left, blk(nxt, 0)),
            (aux(p), left, aux(nxt)),
            (blk(prev, 0), right, blk(opp, 0)),
            (blk(nxt, 1), left, blk(opp, 1)),
            (aux(prev), right, aux(opp)),
        )

    def copy(self, k, ref=None):
        ref = self.sent[k][0] if ref is None else ref
        return pltpu.make_async_remote_copy(ref, ref, self.ssem.at[self.row, k], self.rsem.at[self.row, k], device_id=self.sent[k][1], device_id_type=MESH)

    def recv(self, k):
        self.copy(k, self.sent[k][2]).wait_recv()

    def start_own(self):
        for k in range(6):
            self.copy(k).start()

    def forward(self):
        for k in range(3):
            self.recv(k)
            self.copy(k + 6).start()

    def recv_near(self):
        for k in range(3, 6):
            self.recv(k)

    def recv_far(self):
        for k in range(6, 9):
            self.recv(k)

    def wait_sends(self):
        for k in range(9):
            self.copy(k).wait_send()


def kernel(x_h, pos, inv, wdq, wdkv, wkr, gq, gkv, wuq, wqr, wuk, wuv, wout, y_ref,
           x_v, wkr_v, wbuf, h0, h1, hkr, tabs, stat, stat_rx, cq, lat, kr, pt,
           uq_v, qr_v, uk_v, uv_v, kcat, vbuf, qt, s_buf, m_s, l_s, acc_s, o_v, og, ysend, ykeep, yrecv,
           dsem, isem, osem, ssem, rsem, dssem, drsem, psem, assem, arsem, yssem, yrsem):
    c = lax.axis_index("ctx")
    m = lax.axis_index("model")
    x, y, z = c % 4, (c // 4) % 4, c // 16
    s, d = c // GROUP, c % GROUP
    first = m == 0
    sib = {"ctx": c, "model": 1 - m}
    pa, pb = jnp.where(first, z, y), jnp.where(first, y, z)
    sa, sb = jnp.where(first, 16, 4), jnp.where(first, 4, 16)
    yp = y % 2

    def at(idx):
        return {"ctx": idx, "model": m}

    def near(p, stride):
        return at(c + ((p + 1) % 4 - p) * stride), at(c + ((p + 3) % 4 - p) * stride)

    (xr, xl), (ar, al), (br, bl) = near(x, 1), near(pa, sa), near(pb, sb)
    ypair = at(c + 4 - 8 * yp)
    peers = [at(c - d + (d + k) % GROUP) for k in range(1, GROUP)]

    def down_copies(k):
        src = dyn(k, BLK)
        side, dst = k // N_SIDE, dyn(k % N_SIDE, BLK)
        q0 = pl.multiple_of(m * QH, LANES)
        return (
            pltpu.make_async_copy(wdq.at[src, pl.ds(q0, BLK)], wbuf.at[2 * side, dst], dsem.at[0, k]),
            pltpu.make_async_copy(wdq.at[src, pl.ds(pl.multiple_of(q0 + BLK, LANES), QB)], wbuf.at[2 * side + 1, dst, pl.ds(0, QB)], dsem.at[1, k]),
            pltpu.make_async_copy(wdkv.at[src, dyn(m, KH)], wbuf.at[2 * side + 1, dst, pl.ds(QB, KH)], dsem.at[2, k]),
        )

    def start_down(k, _):
        for cp in down_copies(k):
            cp.start()
        return 0

    def out_copy(j):
        return pltpu.make_async_copy(wout.at[:, dyn(j, BLK)], wbuf.at[lax.rem(j, N_SLOTS)], osem.at[lax.rem(j, N_SLOTS)])

    ins = [
        pltpu.make_async_copy(a, b, isem.at[i])
        for i, (a, b) in enumerate((
            (x_h, x_v), (wkr, wkr_v), (wuq.at[:, dyn(d, BLK)], uq_v), (wqr.at[:, dyn(d, QB)], qr_v),
            (wuk.at[:, dyn(d, BLK)], uk_v), (wuv.at[:, dyn(d, BLK)], uv_v),
        ))
    ]
    for cp in ins[:2]:
        cp.start()
    lax.fori_loop(0, N_DOWN, start_down, 0)
    for cp in ins[2:]:
        cp.start()
    for j in range(N_EARLY, N_SLOTS):
        out_copy(j).start()

    sem = pltpu.get_barrier_semaphore()
    greet = peers + [ar, al, br, bl, sib]
    for dev in greet:
        pl.semaphore_signal(sem, inc=1, device_id=dev, device_id_type=MESH)

    ang = inv[...] * pos[...].astype(F32)
    cos_f, sin_f = jnp.cos(ang), jnp.sin(ang)
    tabs[...] = jnp.transpose(jnp.concatenate([cos_f, cos_f, -sin_f, sin_f], axis=0))
    cs = jnp.transpose(jnp.concatenate([cos_f, sin_f], axis=0))

    def pack(v):
        return jnp.concatenate([v[:HALF_SPAN], v[HALF_SPAN:]], axis=-1)

    pt[m, yp, x] = pack(jnp.where(first, cs[:SPAN], cs[SPAN:]))

    h0[...] = jnp.zeros_like(h0)
    h1[...] = jnp.zeros_like(h1)
    hkr[...] = jnp.zeros_like(hkr)
    for cp in ins[:2]:
        cp.wait()

    def down(k, _):
        for cp in down_copies(k):
            cp.wait()
        side, rows = k // N_SIDE, dyn(k % N_SIDE, BLK)
        xb = x_v[:, dyn(k, BLK)]
        h0[...] += dot(xb, wbuf[2 * side, rows])
        h1[...] += dot(xb, wbuf[2 * side + 1, rows])
        hkr[...] += dot_dims(xb, wkr_v[:, dyn(k, BLK)], 1, 1)
        return 0

    lax.fori_loop(0, N_DOWN, down, 0)
    for j in range(N_EARLY):
        out_copy(j).start()

    h_q = jnp.concatenate([h0[...], h1[:, :QB]], axis=-1)
    h_kv = h1[:, QB:]
    own_q = jnp.sum(h_q * h_q, axis=-1, keepdims=True)
    own_kv = jnp.sum(h_kv * h_kv, axis=-1, keepdims=True)
    stat[...] = jnp.where(iota((TOK, LANES), 1) < TOK, own_q, own_kv)
    pl.semaphore_wait(sem, len(greet))
    st = pltpu.make_async_remote_copy(stat, stat_rx, psem.at[0], psem.at[1], device_id=sib, device_id_type=MESH)
    st.start()

    k_raw = hkr[...]
    swapped = jnp.concatenate([k_raw[:, SPAN:], k_raw[:, :SPAN]], axis=-1)
    k_rot = k_raw * tabs[:, :TOK] + swapped * tabs[:, TOK:]
    kr[m, pa, pb, x] = pack(jnp.where(first, k_rot[:SPAN], k_rot[SPAN:])).astype(BF)

    st.wait()
    tot_q = own_q + stat_rx[:, :1]
    tot_kv = own_kv + stat_rx[:, TOK:TOK + 1]
    nq, nk = QH // LANES, KH // LANES
    g_q = jnp.concatenate([gq[pl.ds(nq * m + i, 1), :] for i in range(nq)], axis=-1)
    g_kv = jnp.concatenate([gkv[pl.ds(nk * m + i, 1), :] for i in range(nk)], axis=-1)
    c_q = (h_q * lax.rsqrt(tot_q / Q_RANK + NORM_EPS) * g_q).astype(BF)
    c_kv = (h_kv * lax.rsqrt(tot_kv / KV_RANK + NORM_EPS) * g_kv).astype(BF)
    for half in range(2):
        lat[m, half, pa, pb, x] = c_kv[SPAN * half:SPAN * half + SPAN]
        cq[m, half, yp, x] = c_q[SPAN * half:SPAN * half + SPAN]

    def share(ref, k):
        return pltpu.make_async_remote_copy(ref, ref, dssem.at[k], drsem.at[k], device_id=sib, device_id_type=MESH)

    def row_ring(b, row):
        return Ring(lambda p, h: lat.at[m, h, p, b], lambda p: kr.at[m, p, b], pa, ar, al, ssem, rsem, row)

    r1 = Ring(lambda p, h: lat.at[m, h, pa, pb, p], lambda p: kr.at[m, pa, pb, p], x, xr, xl, ssem, rsem, 0)
    r2 = Ring(lambda p, h: lat.at[m, h, pa, p], lambda p: kr.at[m, pa, p], pb, br, bl, ssem, rsem, 1)
    rq = Ring(lambda p, h: cq.at[m, h, :, p], lambda p: pt.at[m, :, p], x, xr, xl, ssem, rsem, 2)
    r3 = [row_ring((pb + k) % 4, 3 + k) for k in range(4)]
    nxt, prev, opp = (pa + 1) % 4, (pa + 3) % 4, (pa + 2) % 4

    def pair_copies(par):
        return [
            pltpu.make_async_remote_copy(ref, ref, psem.at[2 + i], psem.at[4 + i], device_id=ypair, device_id_type=MESH)
            for i, ref in enumerate((cq.at[m, :, par, x], pt.at[m, par, x]))
        ]

    def shares(core, planes):
        refs = [cq.at[core], pt.at[core]]
        for p in planes:
            refs += [lat.at[core, :, p], kr.at[core, p]]
        return [share(ref, k) for k, ref in enumerate(refs)]

    mine = shares(m, (pa, prev, nxt, opp))

    r1.start_own()
    for cp in pair_copies(yp):
        cp.start()
    r1.forward()
    r1.recv_near()
    r1.recv_far()
    r2.start_own()
    r3[0].start_own()
    for cp in pair_copies(1 - yp):
        cp.wait_recv()
    rq.start_own()
    r2.forward()
    r2.recv_near()
    r3[1].start_own()
    r3[3].start_own()
    r3[0].forward()
    rq.forward()
    r2.recv_far()
    r3[2].start_own()
    for cp in mine[2:4]:
        cp.start()
    rq.recv_near()
    rq.recv_far()
    for cp in mine[:2]:
        cp.start()
    r3[1].forward()
    r3[3].forward()
    r3[2].forward()
    for r in r3:
        r.recv_near()
    for cp in mine[4:8]:
        cp.start()

    theirs = shares(1 - m, (0, 0, 0, 0))
    for cp in theirs[:2]:
        cp.wait_recv()
    for cp in ins[2:4]:
        cp.wait()
    t = pt[...].reshape(2 * LANES, LANES)
    grp = iota((2 * LANES, LANES), 1) // SPAN

    def both(shift):
        parts = []
        for extra in (0, TOK):
            v = pltpu.roll(t, (shift + extra) % LANES, 1) if shift + extra else t
            r = v
            for g in range(1, 4):
                r = jnp.where(grp == g, pltpu.roll(v, SPAN * g, 1), r)
            parts.append(r.reshape(HALF_SPAN, HALF_SPAN, LANES))
        return jnp.concatenate(parts, axis=1).reshape(BLK, LANES)

    lower = iota((BLK, LANES), 1) % TOK < SPAN
    cos_t = both(0)
    sin_t = both(LANES - SPAN)
    sin_t = jnp.where(lower, -sin_t, sin_t)
    c0, c1 = cq[0].reshape(BLK, QH), cq[1].reshape(BLK, QH)
    for p in range(2):
        wide, thin = slice(QB * p, QB * p + QB), slice(LANES * p, LANES * p + LANES)
        qn = dot(c0, uq_v[:QH, wide]) + dot(c1, uq_v[QH:, wide])
        qr = dot(c0, qr_v[:QH, thin]) + dot(c1, qr_v[QH:, thin])
        rot = jnp.where(lower, pltpu.roll(qr, LANES - SPAN, 1), pltpu.roll(qr, SPAN, 1))
        qn_t = jnp.transpose(qn).astype(BF)
        qr_t = jnp.transpose(qr * cos_t + rot * sin_t).astype(BF)
        for a in range(2):
            qt[2 * p + a, :LANES, :] = qn_t[LANES * a:LANES * a + LANES]
            qt[2 * p + a, LANES:QK_DIM, :] = qr_t[TOK * a:TOK * a + TOK]

    for r in r3:
        r.recv_far()
    for cp in mine[8:]:
        cp.start()
    for cp in ins[4:]:
        cp.wait()
    for cp in theirs[2:]:
        cp.wait_recv()

    for half in range(2):
        if half == 0:
            k2 = kr[0].reshape(ROWS_H // 2, LANES).astype(F32)
        else:
            k2 = jnp.concatenate([kr[1, :, zz].reshape(QB, LANES) for zz in range(4)], axis=0).astype(F32)
        lo = k2.reshape(TOK, HALF_SPAN, LANES)[:, :, :TOK]
        hi = pltpu.roll(k2, TOK, 1).reshape(TOK, HALF_SPAN, LANES)[:, :, :TOK]
        k3 = jnp.concatenate([lo, hi], axis=1).astype(BF).reshape(ROWS_H, TOK)
        for a in range(2):
            kcat[a, ROWS_H * half:ROWS_H * half + ROWS_H, LANES:QK_DIM] = k3

    nlow = s // 2 + 1

    def place(i):
        low = i < nlow
        b = jnp.where(low, i, i - nlow)
        return low, jnp.where(low, 0, 1), b, jnp.where(b < 4, b, 11 - b)

    def attn_sends(p):
        return [
            pltpu.make_async_remote_copy(
                o_v.at[:, (d + k) % GROUP, :, dyn(p, QB)], og.at[:, :, dyn(2 * d + p, QB)],
                assem.at[p, k - 1], arsem.at[p, k - 1], device_id=peers[k - 1], device_id_type=MESH)
            for k in range(1, GROUP)
        ]

    def pair(p, _):
        pc = dyn(p, QB)

        def up(i, _):
            half, zz = i // 4, i % 4
            a0 = lat[0, half, zz].reshape(BLK, KH)
            a1 = lat[1, half, :, zz].reshape(BLK, KH)
            rows = dyn(i, BLK)
            kn = (dot(a0, uk_v[:KH, pc]) + dot(a1, uk_v[KH:, pc])).astype(BF)
            kcat[0, rows, :LANES] = kn[:, :LANES]
            kcat[1, rows, :LANES] = kn[:, LANES:]
            vbuf[rows, :] = (dot(a0, uv_v[:KH, pc]) + dot(a1, uv_v[KH:, pc])).astype(BF)
            return 0

        lax.fori_loop(0, 8, up, 0)
        m_s[...] = jnp.full(m_s.shape, NEG_BIG, F32)
        l_s[...] = jnp.zeros_like(l_s)
        acc_s[...] = jnp.zeros_like(acc_s)

        def scores(i, a):
            _, qb, _, kb = place(i)
            return dot(kcat[a, dyn(kb, BLK), :QK_DIM], qt[2 * p + a, :, dyn(qb, QB)])

        for a in range(2):
            s_buf[a] = scores(0, a)

        def tile(i, _):
            low, qb, b, kb = place(i)

            @pl.when(b == jnp.where(low, s // 2, 7 - s // 2))
            def _():
                r = iota((BLK, 1), 0)
                cc = iota((1, QB), 1)
                k_idx = BLK * b + jnp.where(b < 4, r, (15 - r // SPAN) * SPAN + r % SPAN)
                q_idx = jnp.where(low, QB * s + cc, SPAN * (LANES - 1 - GROUP * s - cc // SPAN) + cc % SPAN)
                allowed = k_idx <= q_idx
                for a in range(2):
                    s_buf[a] = jnp.where(allowed, s_buf[a], NEG_BIG)

            after = jnp.minimum(i + 1, N_TILES - 1)
            for a in range(2):
                sc = s_buf[a]
                m_old = m_s[a, qb, :1, :]
                m_new = jnp.maximum(m_old, jnp.max(sc, axis=0, keepdims=True))
                e = jnp.exp2((sc - m_new) * EXP_SCALE)
                alpha = jnp.exp2((m_old - m_new) * EXP_SCALE)
                l_s[a, qb, :1, :] = l_s[a, qb, :1, :] * alpha + jnp.sum(e, axis=0, keepdims=True)
                s_buf[a] = scores(after, a)
                pv = dot_dims(vbuf[dyn(kb, BLK), LANES * a:LANES * a + LANES], e.astype(BF), 0, 0)
                acc_s[a, qb] = acc_s[a, qb] * alpha + pv
                m_s[a, qb, :1, :] = m_new
            return 0

        lax.fori_loop(0, N_TILES, tile, 0)
        for a in range(2):
            for qb in range(2):
                ot = acc_s[a, qb] / l_s[a, qb, :1, :]
                o_v[qb, :, :, dyn(2 * p + a, LANES)] = jnp.transpose(ot).astype(BF).reshape(GROUP, SPAN, LANES)
        for cp in attn_sends(p):
            cp.start()
        return 0

    lax.fori_loop(0, 2, pair, 0)
    og[:, :, dyn(d, BLK)] = o_v[:, d]

    for r in [r1, r2, rq] + r3:
        r.wait_sends()
    for cp in pair_copies(yp) + mine:
        cp.wait_send()
    for p in range(2):
        for cp in attn_sends(p):
            cp.wait()

    def y_copy(j):
        return pltpu.make_async_remote_copy(ysend.at[j], yrecv.at[j], yssem.at[j], yrsem.at[j], device_id=sib, device_id_type=MESH)

    def finish(j):
        y_copy(j).wait()
        y_ref[:, dyn(j, BLK)] = (ykeep[j] + yrecv[j]).astype(BF)

    def out_step(j, _):
        out_copy(j).wait()
        acc = dot(og[...].reshape(TOK, KEYS), wbuf[lax.rem(j, N_SLOTS)])
        ykeep[j] = jnp.where(first, acc[:SPAN], acc[SPAN:])
        ysend[j] = jnp.where(first, acc[SPAN:], acc[:SPAN])
        y_copy(j).start()

        @pl.when(j + N_SLOTS < N_OUT)
        def _():
            out_copy(j + N_SLOTS).start()

        @pl.when(j > 0)
        def _():
            finish(j - 1)
        return 0

    lax.fori_loop(0, N_OUT, out_step, 0)
    finish(N_OUT - 1)


def fused(x, pos, inv, wdq, wdkv, wkr, gq, gkv, wuq, wqr, wuk, wuv, wout):
    vm = pl.BlockSpec(memory_space=pltpu.VMEM)
    hbm = pl.BlockSpec(memory_space=pl.ANY)
    v, dma = pltpu.VMEM, pltpu.SemaphoreType.DMA
    state = v((2, 2, 8, QB), F32)
    part = v((N_OUT, SPAN, BLK), F32)
    return pl.pallas_call(
        kernel,
        name="mla_prefill",
        out_shape=jax.ShapeDtypeStruct((SPAN, HIDDEN), BF),
        in_specs=[hbm, vm, vm, hbm, hbm, hbm, vm, vm] + [hbm] * 5,
        out_specs=vm,
        scratch_shapes=[
            v((TOK, HIDDEN), BF), v((TOK, HIDDEN), BF), v((N_SLOTS, KEYS, BLK), BF),
            v((TOK, BLK), F32), v((TOK, BLK), F32), v((TOK, TOK), F32), v((TOK, LANES), F32), v((TOK, LANES), F32), v((TOK, LANES), F32),
            v((2, 2, 2, 4, SPAN, QH), BF), v((2, 2, 4, 4, 4, SPAN, KH), BF), v((2, 4, 4, 4, HALF_SPAN, LANES), BF), v((2, 2, 4, HALF_SPAN, LANES), F32),
            v((Q_RANK, BLK), BF), v((Q_RANK, QB), BF), v((KV_RANK, BLK), BF), v((KV_RANK, BLK), BF),
            v((2, KEYS, QB), BF), v((KEYS, QB), BF), v((4, QK_DIM, BLK), BF), v((2, BLK, QB), F32),
            state, state, v((2, 2, LANES, QB), F32), v((2, GROUP, SPAN, BLK), BF), v((2, SPAN, KEYS), BF), part, part, part,
            dma((3, N_DOWN)), dma((6,)), dma((N_SLOTS,)), dma((7, 9)), dma((7, 9)), dma((10,)), dma((10,)), dma((6,)),
            dma((2, 7)), dma((2, 7)), dma((N_OUT,)), dma((N_OUT,)),
        ],
        compiler_params=pltpu.CompilerParams(collective_id=0, has_side_effects=True, vmem_limit_bytes=LIMIT),
    )(x, pos, inv, wdq, wdkv, wkr, gq, gkv, wuq, wqr, wuk, wuv, wout)


def solution(mesh):
    freq = ROPE_BASE ** (-np.arange(SPAN) * 2.0 / TOK)
    inv = np.repeat(freq.astype(np.float32)[:, None], TOK, axis=1)

    def local(x_tokens, positions, w_dq, gain_q, w_uq, w_qr, w_dkv, gain_kv, w_kr, w_uk, w_uv, w_out):
        return fused(x_tokens, positions[None], inv, w_dq, w_dkv, w_kr.T, gain_q.reshape(-1, LANES), gain_kv.reshape(-1, LANES), w_uq, w_qr, w_uk, w_uv, w_out)

    in_specs = (P(('dp', 'ctx'), None), P(('dp', 'ctx')), P(), P(), P(None, 'model'), P(None, 'model'), P(), P(), P(), P(None, 'model'), P(None, 'model'), P('model', None))
    out_specs = P(('dp', 'ctx', 'model'), None)
    return jax.shard_map(local, mesh=mesh, in_specs=in_specs, out_specs=out_specs, check_vma=False)
```

```python
import math

import numpy as np
import jax
import jax.numpy as jnp
from jax import lax
from jax.experimental import pallas as pl
from jax.experimental.pallas import tpu as pltpu
from jax.sharding import PartitionSpec as P

NORM_EPS = 1e-6
ROPE_BASE = 10000.0
NEG_BIG = -1e30
MESH = pl.DeviceIdType.MESH
BF = jnp.bfloat16
F32 = jnp.float32

HIDDEN = 7168
Q_RANK = 1536
KV_RANK = 512
TOK = 64
SPAN = 32
HALF_SPAN = SPAN // 2
LANES = 128
QH = Q_RANK // 2
KH = KV_RANK // 2
BLK = 512
QB = 256
QK_DIM = 192
KEYS = 4096
ROWS_H = KEYS // 2
N_DOWN = HIDDEN // BLK
N_OUT = HIDDEN // BLK
N_SLOTS = 16
N_TILES = 9
GROUP = 8
EXP_SCALE = QK_DIM ** -0.5 * math.log2(math.e)
LIMIT = 66 * 10 ** 6


def dot(a, b):
    return jnp.dot(a, b, preferred_element_type=F32)


def dot_dims(a, b, ca, cb):
    return lax.dot_general(a, b, (((ca,), (cb,)), ((), ())), preferred_element_type=F32)


def iota(shape, axis):
    return lax.broadcasted_iota(jnp.int32, shape, axis)


def dyn(i, width):
    return pl.ds(pl.multiple_of(i * width, math.gcd(width, BLK)), width)


class Direct:
    def __init__(self, blk, aux, p, devs, ssem, rsem, row):
        self.ssem, self.rsem, self.row = ssem, rsem, row
        self.sent = []
        for off, dev in zip((1, 3, 2), devs):
            src = (p - off + 4) % 4
            self.sent += [(blk(p, 0), dev, blk(src, 0)), (blk(p, 1), dev, blk(src, 1)), (aux(p), dev, aux(src))]

    def copy(self, k, ref=None):
        ref = self.sent[k][0] if ref is None else ref
        return pltpu.make_async_remote_copy(ref, ref, self.ssem.at[self.row, k], self.rsem.at[self.row, k], device_id=self.sent[k][1], device_id_type=MESH)

    def start_own(self):
        for k in range(9):
            self.copy(k).start()

    def recv_all(self):
        for k in range(9):
            self.copy(k, self.sent[k][2]).wait_recv()

    def wait_sends(self):
        for k in range(9):
            self.copy(k).wait_send()


class Ring:
    def __init__(self, blk, aux, p, right, left, ssem, rsem, row):
        prev, nxt, opp = (p + 3) % 4, (p + 1) % 4, (p + 2) % 4
        self.ssem, self.rsem, self.row = ssem, rsem, row
        self.sent = (
            (blk(p, 0), right, blk(prev, 0)),
            (blk(p, 1), left, blk(nxt, 1)),
            (aux(p), right, aux(prev)),
            (blk(p, 1), right, blk(prev, 1)),
            (blk(p, 0), left, blk(nxt, 0)),
            (aux(p), left, aux(nxt)),
            (blk(prev, 0), right, blk(opp, 0)),
            (blk(nxt, 1), left, blk(opp, 1)),
            (aux(prev), right, aux(opp)),
        )

    def copy(self, k, ref=None):
        ref = self.sent[k][0] if ref is None else ref
        return pltpu.make_async_remote_copy(ref, ref, self.ssem.at[self.row, k], self.rsem.at[self.row, k], device_id=self.sent[k][1], device_id_type=MESH)

    def recv(self, k):
        self.copy(k, self.sent[k][2]).wait_recv()

    def start_own(self):
        for k in range(6):
            self.copy(k).start()

    def forward(self, keys=(0, 1, 2)):
        for k in keys:
            self.recv(k)
            self.copy(k + 6).start()

    def recv_near(self):
        for k in range(3, 6):
            self.recv(k)

    def recv_far(self):
        for k in range(6, 9):
            self.recv(k)

    def wait_sends(self):
        for k in range(9):
            self.copy(k).wait_send()


def kernel(x_h, pos, inv, wdq, wdkv, wkr, gq, gkv, wuq, wqr, wuk, wuv, wout, y_ref,
           x_v, wkr_v, wbuf, h0, h1, hkr, tabs, stat, stat_rx, cq, lat, kr, pt,
           uq_v, qr_v, uk_v, uv_v, kcat, vbuf, qt, s_buf, m_s, l_s, acc_s, o_v, og, ysend, ykeep, yrecv,
           dsem, isem, osem, ssem, rsem, dssem, drsem, psem, assem, arsem, yssem, yrsem):
    c = lax.axis_index("ctx")
    m = lax.axis_index("model")
    x, y, z = c % 4, (c // 4) % 4, c // 16
    s, d = c // GROUP, c % GROUP
    first = m == 0
    sib = {"ctx": c, "model": 1 - m}
    pa, pb = jnp.where(first, z, y), jnp.where(first, y, z)
    sa, sb = jnp.where(first, 16, 4), jnp.where(first, 4, 16)
    yp = y % 2

    def at(idx):
        return {"ctx": idx, "model": m}

    def near(p, stride):
        return at(c + ((p + 1) % 4 - p) * stride), at(c + ((p + 3) % 4 - p) * stride)

    (xr, xl), (ar, al), (br, bl) = near(x, 1), near(pa, sa), near(pb, sb)
    xo = at(c + (x + 2) % 4 - x)
    ypair = at(c + 4 - 8 * yp)
    peers = [at(c - d + (d + k) % GROUP) for k in range(1, GROUP)]

    def down_copies(k):
        src, dst, slot = pl.ds(2 * k, 2), pl.ds(2 * (k % 4), 2), 2 * (k // 4)
        q0 = pl.multiple_of(m * QH, LANES)
        return (
            pltpu.make_async_copy(wdq.at[src, :, pl.ds(q0, BLK)], wbuf.at[slot, dst], dsem.at[0, k]),
            pltpu.make_async_copy(wdq.at[src, :, pl.ds(pl.multiple_of(q0 + BLK, LANES), QB)], wbuf.at[slot + 1, dst, :, pl.ds(0, QB)], dsem.at[1, k]),
            pltpu.make_async_copy(wdkv.at[src, :, dyn(m, KH)], wbuf.at[slot + 1, dst, :, pl.ds(QB, KH)], dsem.at[2, k]),
        )

    def start_down(k, _):
        for cp in down_copies(k):
            cp.start()
        return 0

    def out_copy(t):
        slot = lax.rem(t, N_SLOTS)
        return pltpu.make_async_copy(wout.at[:, t // N_OUT, :, dyn(lax.rem(t, N_OUT), BLK)], wbuf.at[slot], osem.at[slot])

    ins = [
        pltpu.make_async_copy(a, b, isem.at[i])
        for i, (a, b) in enumerate((
            (x_h, x_v), (wkr, wkr_v), (wuq.at[:, dyn(d, BLK)], uq_v), (wqr.at[:, dyn(d, QB)], qr_v),
            (wuk.at[:, dyn(d, BLK)], uk_v), (wuv.at[:, dyn(d, BLK)], uv_v),
        ))
    ]
    for cp in ins[:2]:
        cp.start()
    lax.fori_loop(0, N_DOWN, start_down, 0)

    sem = pltpu.get_barrier_semaphore()
    greet = peers + [ar, al, br, bl, sib]
    for dev in greet:
        pl.semaphore_signal(sem, inc=1, device_id=dev, device_id_type=MESH)

    ang = inv[...] * pos[...].astype(F32)
    cos_f, sin_f = jnp.cos(ang), jnp.sin(ang)
    tabs[...] = jnp.transpose(jnp.concatenate([cos_f, cos_f, -sin_f, sin_f], axis=0))
    cs = jnp.transpose(jnp.concatenate([cos_f, sin_f], axis=0))

    def pack(v):
        return jnp.concatenate([v[:HALF_SPAN], v[HALF_SPAN:]], axis=-1)

    pt[m, yp, x] = pack(jnp.where(first, cs[:SPAN], cs[SPAN:]))

    h0[...] = jnp.zeros_like(h0)
    h1[...] = jnp.zeros_like(h1)
    hkr[...] = jnp.zeros_like(hkr)
    for cp in ins[:2]:
        cp.wait()

    def down(k, _):
        for cp in down_copies(k):
            cp.wait()
        slot, rows = 2 * (k // 4), pl.ds(2 * (k % 4), 2)
        xb = x_v[:, dyn(k, BLK)]
        h0[...] += dot(xb, wbuf[slot, rows].reshape(BLK, BLK))
        h1[...] += dot(xb, wbuf[slot + 1, rows].reshape(BLK, BLK))
        hkr[...] += dot_dims(xb, wkr_v[:, dyn(k, BLK)], 1, 1)
        return 0

    lax.fori_loop(0, N_DOWN, down, 0)
    for cp in ins[2:]:
        cp.start()
    for j in range(N_SLOTS):
        out_copy(j).start()

    h_q = jnp.concatenate([h0[...], h1[:, :QB]], axis=-1)
    h_kv = h1[:, QB:]
    own_q = jnp.sum(h_q * h_q, axis=-1, keepdims=True)
    own_kv = jnp.sum(h_kv * h_kv, axis=-1, keepdims=True)
    stat[...] = jnp.where(iota((TOK, LANES), 1) < TOK, own_q, own_kv)
    pl.semaphore_wait(sem, len(greet))
    st = pltpu.make_async_remote_copy(stat, stat_rx, psem.at[0], psem.at[1], device_id=sib, device_id_type=MESH)
    st.start()

    k_raw = hkr[...]
    swapped = jnp.concatenate([k_raw[:, SPAN:], k_raw[:, :SPAN]], axis=-1)
    k_rot = k_raw * tabs[:, :TOK] + swapped * tabs[:, TOK:]
    kr[m, pa, pb, x] = pack(jnp.where(first, k_rot[:SPAN], k_rot[SPAN:])).astype(BF)

    st.wait()
    tot_q = own_q + stat_rx[:, :1]
    tot_kv = own_kv + stat_rx[:, TOK:TOK + 1]
    nq, nk = QH // LANES, KH // LANES
    g_q = jnp.concatenate([gq[pl.ds(nq * m + i, 1), :] for i in range(nq)], axis=-1)
    g_kv = jnp.concatenate([gkv[pl.ds(nk * m + i, 1), :] for i in range(nk)], axis=-1)
    c_q = (h_q * lax.rsqrt(tot_q / Q_RANK + NORM_EPS) * g_q).astype(BF)
    c_kv = (h_kv * lax.rsqrt(tot_kv / KV_RANK + NORM_EPS) * g_kv).astype(BF)
    for half in range(2):
        lat[m, half, pa, pb, x] = c_kv[SPAN * half:SPAN * half + SPAN]
        cq[m, half, yp, x] = c_q[SPAN * half:SPAN * half + SPAN]

    def share(ref, k):
        return pltpu.make_async_remote_copy(ref, ref, dssem.at[k], drsem.at[k], device_id=sib, device_id_type=MESH)

    def row_ring(b, row):
        return Ring(lambda p, h: lat.at[m, h, p, b], lambda p: kr.at[m, p, b], pa, ar, al, ssem, rsem, row)

    r1 = Direct(lambda p, h: lat.at[m, h, pa, pb, p], lambda p: kr.at[m, pa, pb, p], x, (xr, xl, xo), ssem, rsem, 0)
    r2 = Ring(lambda p, h: lat.at[m, h, pa, p], lambda p: kr.at[m, pa, p], pb, br, bl, ssem, rsem, 1)
    rq = Ring(lambda p, h: cq.at[m, h, :, p], lambda p: pt.at[m, :, p], x, xr, xl, ssem, rsem, 2)
    r3 = [row_ring((pb + k) % 4, 3 + k) for k in range(4)]
    nxt, prev, opp = (pa + 1) % 4, (pa + 3) % 4, (pa + 2) % 4

    def pair_copies(par):
        return [
            pltpu.make_async_remote_copy(ref, ref, psem.at[2 + i], psem.at[4 + i], device_id=ypair, device_id_type=MESH)
            for i, ref in enumerate((cq.at[m, :, par, x], pt.at[m, par, x]))
        ]

    def shares(core, own, planes, rows):
        refs = [cq.at[core], pt.at[core], lat.at[core, :, own], kr.at[core, own]]
        for b in rows:
            for p in planes:
                refs += [lat.at[core, :, p, b], kr.at[core, p, b]]
        return [share(ref, k) for k, ref in enumerate(refs)]

    mine = shares(m, pa, (prev, nxt, opp), [(pb + k) % 4 for k in range(4)])

    def start_shares(first_k, count):
        for cp in mine[first_k:first_k + count]:
            cp.start()

    def row_near(k):
        r3[k].forward()
        r3[k].recv_near()
        start_shares(4 + 6 * k, 4)

    def row_far(k):
        r3[k].recv_far()
        start_shares(8 + 6 * k, 2)

    r1.start_own()
    for cp in pair_copies(yp):
        cp.start()
    r1.recv_all()
    r2.start_own()
    for cp in pair_copies(1 - yp):
        cp.wait_recv()
    rq.start_own()
    r2.forward((0,))
    r3[0].start_own()
    r2.forward((1, 2))
    r2.recv_near()
    r3[1].start_own()
    r3[3].start_own()
    row_near(0)
    r2.recv_far()
    r3[2].start_own()
    start_shares(2, 2)
    rq.forward()
    row_near(1)
    row_near(3)
    rq.recv_near()
    rq.recv_far()
    start_shares(0, 2)
    row_near(2)
    row_far(0)

    theirs = shares(1 - m, 0, (0, 0, 0), range(4))
    for cp in theirs[:2]:
        cp.wait_recv()
    for cp in ins[2:4]:
        cp.wait()
    t = pt[...].reshape(2 * LANES, LANES)
    grp = iota((2 * LANES, LANES), 1) // SPAN

    def both(shift):
        parts = []
        for extra in (0, TOK):
            v = pltpu.roll(t, (shift + extra) % LANES, 1) if shift + extra else t
            r = v
            for g in range(1, 4):
                r = jnp.where(grp == g, pltpu.roll(v, SPAN * g, 1), r)
            parts.append(r.reshape(HALF_SPAN, HALF_SPAN, LANES))
        return jnp.concatenate(parts, axis=1).reshape(BLK, LANES)

    lower = iota((BLK, LANES), 1) % TOK < SPAN
    cos_t = both(0)
    sin_t = both(LANES - SPAN)
    sin_t = jnp.where(lower, -sin_t, sin_t)
    c0, c1 = cq[0].reshape(BLK, QH), cq[1].reshape(BLK, QH)
    for p in range(2):
        wide, thin = slice(QB * p, QB * p + QB), slice(LANES * p, LANES * p + LANES)
        qn = dot(c0, uq_v[:QH, wide]) + dot(c1, uq_v[QH:, wide])
        qr = dot(c0, qr_v[:QH, thin]) + dot(c1, qr_v[QH:, thin])
        rot = jnp.where(lower, pltpu.roll(qr, LANES - SPAN, 1), pltpu.roll(qr, SPAN, 1))
        qn_t = jnp.transpose(qn).astype(BF)
        qr_t = jnp.transpose(qr * cos_t + rot * sin_t).astype(BF)
        for a in range(2):
            qt[2 * p + a, :LANES, :] = qn_t[LANES * a:LANES * a + LANES]
            qt[2 * p + a, LANES:QK_DIM, :] = qr_t[TOK * a:TOK * a + TOK]

    for k in (1, 3, 2):
        row_far(k)
    for cp in ins[4:]:
        cp.wait()
    for cp in theirs[2:]:
        cp.wait_recv()

    for half in range(2):
        if half == 0:
            k2 = kr[0].reshape(ROWS_H // 2, LANES).astype(F32)
        else:
            k2 = jnp.concatenate([kr[1, :, zz].reshape(QB, LANES) for zz in range(4)], axis=0).astype(F32)
        lo = k2.reshape(TOK, HALF_SPAN, LANES)[:, :, :TOK]
        hi = pltpu.roll(k2, TOK, 1).reshape(TOK, HALF_SPAN, LANES)[:, :, :TOK]
        k3 = jnp.concatenate([lo, hi], axis=1).astype(BF).reshape(ROWS_H, TOK)
        for a in range(2):
            kcat[a, ROWS_H * half:ROWS_H * half + ROWS_H, LANES:QK_DIM] = k3

    nlow = s // 2 + 1

    def place(i):
        low = i < nlow
        b = jnp.where(low, i, i - nlow)
        return low, jnp.where(low, 0, 1), b, jnp.where(b < 4, b, 11 - b)

    def attn_sends(p):
        return [
            pltpu.make_async_remote_copy(
                o_v.at[p, :, (d + k) % GROUP], og.at[p, :, :, dyn(d, QB)],
                assem.at[p, k - 1], arsem.at[p, k - 1], device_id=peers[k - 1], device_id_type=MESH)
            for k in range(1, GROUP)
        ]

    def pair(p, _):
        pc = dyn(p, QB)

        def up(i, _):
            half, zz = i // 2, 2 * (i % 2)
            a0 = lat[0, half, pl.ds(zz, 2)].reshape(2 * BLK, KH)
            a1 = jnp.concatenate([lat[1, half, :, zz + k].reshape(BLK, KH) for k in range(2)], axis=0)
            rows = pl.ds(pl.multiple_of(i * 2 * BLK, BLK), 2 * BLK)
            kn = (dot(a0, uk_v[:KH, pc]) + dot(a1, uk_v[KH:, pc])).astype(BF)
            kcat[0, rows, :LANES] = kn[:, :LANES]
            kcat[1, rows, :LANES] = kn[:, LANES:]
            vbuf[rows, :] = (dot(a0, uv_v[:KH, pc]) + dot(a1, uv_v[KH:, pc])).astype(BF)
            return 0

        lax.fori_loop(0, 4, up, 0)
        m_s[...] = jnp.full(m_s.shape, NEG_BIG, F32)
        l_s[...] = jnp.zeros_like(l_s)
        acc_s[...] = jnp.zeros_like(acc_s)

        def scores(i, a):
            _, qb, _, kb = place(i)
            return dot(kcat[a, dyn(kb, BLK), :QK_DIM], qt[2 * p + a, :, dyn(qb, QB)])

        for a in range(2):
            s_buf[a] = scores(0, a)

        def tile(i, _):
            low, qb, b, kb = place(i)

            @pl.when(b == jnp.where(low, s // 2, 7 - s // 2))
            def _():
                r = iota((BLK, 1), 0)
                cc = iota((1, QB), 1)
                k_idx = BLK * b + jnp.where(b < 4, r, (15 - r // SPAN) * SPAN + r % SPAN)
                q_idx = jnp.where(low, QB * s + cc, SPAN * (LANES - 1 - GROUP * s - cc // SPAN) + cc % SPAN)
                allowed = k_idx <= q_idx
                for a in range(2):
                    s_buf[a] = jnp.where(allowed, s_buf[a], NEG_BIG)

            after = jnp.minimum(i + 1, N_TILES - 1)
            for a in range(2):
                sc = s_buf[a]
                m_old = m_s[a, qb, :1, :]
                m_new = jnp.maximum(m_old, jnp.max(sc, axis=0, keepdims=True))
                e = jnp.exp2((sc - m_new) * EXP_SCALE)
                alpha = jnp.exp2((m_old - m_new) * EXP_SCALE)
                l_s[a, qb, :1, :] = l_s[a, qb, :1, :] * alpha + jnp.sum(e, axis=0, keepdims=True)
                s_buf[a] = scores(after, a)
                pv = dot_dims(vbuf[dyn(kb, BLK), LANES * a:LANES * a + LANES], e.astype(BF), 0, 0)
                acc_s[a, qb] = acc_s[a, qb] * alpha + pv
                m_s[a, qb, :1, :] = m_new
            return 0

        lax.fori_loop(0, N_TILES, tile, 0)
        for a in range(2):
            for qb in range(2):
                ot = acc_s[a, qb] / l_s[a, qb, :1, :]
                o_v[p, qb, :, :, LANES * a:LANES * a + LANES] = jnp.transpose(ot).astype(BF).reshape(GROUP, SPAN, LANES)
        for cp in attn_sends(p):
            cp.start()
        og[p, :, :, dyn(d, QB)] = o_v[p, :, d]
        return 0

    lax.fori_loop(0, 2, pair, 0)

    for r in [r1, r2, rq] + r3:
        r.wait_sends()
    for cp in pair_copies(yp) + mine:
        cp.wait_send()
    for cp in attn_sends(0):
        cp.wait()

    def y_copy(j):
        return pltpu.make_async_remote_copy(ysend.at[j], yrecv.at[j], yssem.at[j], yrsem.at[j], device_id=sib, device_id_type=MESH)

    def finish(j):
        y_copy(j).wait()
        y_ref[:, dyn(j, BLK)] = (ykeep[j, :SPAN] + yrecv[j]).astype(BF)

    def half_dot(t):
        out_copy(t).wait()
        return dot(og[t // N_OUT].reshape(TOK, ROWS_H), wbuf[lax.rem(t, N_SLOTS)].reshape(ROWS_H, BLK))

    def refill(t):
        @pl.when(t + N_SLOTS < 2 * N_OUT)
        def _():
            out_copy(t + N_SLOTS).start()

    def first_half(j, _):
        ykeep[j] = half_dot(j)
        refill(j)
        return 0

    lax.fori_loop(0, N_OUT, first_half, 0)
    for cp in attn_sends(1):
        cp.wait()

    def second_half(j, _):
        acc = ykeep[j] + half_dot(j + N_OUT)
        ykeep[j, :SPAN] = jnp.where(first, acc[:SPAN], acc[SPAN:])
        ysend[j] = jnp.where(first, acc[SPAN:], acc[:SPAN])
        y_copy(j).start()
        refill(j + N_OUT)

        @pl.when(j > 0)
        def _():
            finish(j - 1)
        return 0

    lax.fori_loop(0, N_OUT, second_half, 0)
    finish(N_OUT - 1)


def fused(x, pos, inv, wdq, wdkv, wkr, gq, gkv, wuq, wqr, wuk, wuv, wout):
    vm = pl.BlockSpec(memory_space=pltpu.VMEM)
    hbm = pl.BlockSpec(memory_space=pl.ANY)
    v, dma = pltpu.VMEM, pltpu.SemaphoreType.DMA
    state = v((2, 2, 8, QB), F32)
    part = v((N_OUT, SPAN, BLK), F32)
    return pl.pallas_call(
        kernel,
        name="mla_prefill",
        out_shape=jax.ShapeDtypeStruct((SPAN, HIDDEN), BF),
        in_specs=[hbm, vm, vm, hbm, hbm, hbm, vm, vm] + [hbm] * 5,
        out_specs=vm,
        scratch_shapes=[
            v((TOK, HIDDEN), BF), v((TOK, HIDDEN), BF), v((N_SLOTS, GROUP, QB, BLK), BF),
            v((TOK, BLK), F32), v((TOK, BLK), F32), v((TOK, TOK), F32), v((TOK, LANES), F32), v((TOK, LANES), F32), v((TOK, LANES), F32),
            v((2, 2, 2, 4, SPAN, QH), BF), v((2, 2, 4, 4, 4, SPAN, KH), BF), v((2, 4, 4, 4, HALF_SPAN, LANES), BF), v((2, 2, 4, HALF_SPAN, LANES), F32),
            v((Q_RANK, BLK), BF), v((Q_RANK, QB), BF), v((KV_RANK, BLK), BF), v((KV_RANK, BLK), BF),
            v((2, KEYS, QB), BF), v((KEYS, QB), BF), v((4, QK_DIM, BLK), BF), v((2, BLK, QB), F32),
            state, state, v((2, 2, LANES, QB), F32), v((2, 2, GROUP, SPAN, QB), BF), v((2, 2, SPAN, ROWS_H), BF), part, v((N_OUT, TOK, BLK), F32), part,
            dma((3, N_DOWN)), dma((6,)), dma((N_SLOTS,)), dma((7, 9)), dma((7, 9)), dma((28,)), dma((28,)), dma((6,)),
            dma((2, 7)), dma((2, 7)), dma((N_OUT,)), dma((N_OUT,)),
        ],
        compiler_params=pltpu.CompilerParams(collective_id=0, has_side_effects=True, vmem_limit_bytes=LIMIT),
    )(x, pos, inv, wdq, wdkv, wkr, gq, gkv, wuq, wqr, wuk, wuv, wout)


def solution(mesh):
    freq = ROPE_BASE ** (-np.arange(SPAN) * 2.0 / TOK)
    inv = np.repeat(freq.astype(np.float32)[:, None], TOK, axis=1)

    def local(x_tokens, positions, w_dq, gain_q, w_uq, w_qr, w_dkv, gain_kv, w_kr, w_uk, w_uv, w_out):
        return fused(x_tokens, positions[None], inv, w_dq.reshape(-1, QB, Q_RANK), w_dkv.reshape(-1, QB, KV_RANK), w_kr.T, gain_q.reshape(-1, LANES), gain_kv.reshape(-1, LANES), w_uq, w_qr, w_uk, w_uv, w_out.reshape(GROUP, 2, QB, HIDDEN))

    in_specs = (P(('dp', 'ctx'), None), P(('dp', 'ctx')), P(), P(), P(None, 'model'), P(None, 'model'), P(), P(), P(), P(None, 'model'), P(None, 'model'), P('model', None))
    out_specs = P(('dp', 'ctx', 'model'), None)
    return jax.shard_map(local, mesh=mesh, in_specs=in_specs, out_specs=out_specs, check_vma=False)
```

```python
import math

import numpy as np
import jax
import jax.numpy as jnp
from jax import lax
from jax.experimental import pallas as pl
from jax.experimental.pallas import tpu as pltpu
from jax.sharding import PartitionSpec as P

NORM_EPS = 1e-6
ROPE_BASE = 10000.0
NEG_BIG = -1e30
MESH = pl.DeviceIdType.MESH
BF = jnp.bfloat16
F32 = jnp.float32

HIDDEN = 7168
Q_RANK = 1536
KV_RANK = 512
TOK = 64
SPAN = 32
HALF_SPAN = SPAN // 2
LANES = 128
QH = Q_RANK // 2
KH = KV_RANK // 2
BLK = 512
QB = 256
QK_DIM = 192
KEYS = 4096
ROWS_H = KEYS // 2
N_DOWN = HIDDEN // BLK
N_OUT = HIDDEN // BLK
N_SLOTS = 16
LAG = 3
N_TILES = 9
GROUP = 8
EXP_SCALE = QK_DIM ** -0.5 * math.log2(math.e)
LIMIT = 66 * 10 ** 6


def dot(a, b):
    return jnp.dot(a, b, preferred_element_type=F32)


def dot_dims(a, b, ca, cb):
    return lax.dot_general(a, b, (((ca,), (cb,)), ((), ())), preferred_element_type=F32)


def iota(shape, axis):
    return lax.broadcasted_iota(jnp.int32, shape, axis)


def dyn(i, width):
    return pl.ds(pl.multiple_of(i * width, math.gcd(width, BLK)), width)


class Direct:
    def __init__(self, blk, aux, p, devs, ssem, rsem, row):
        self.ssem, self.rsem, self.row = ssem, rsem, row
        self.sent = []
        for off, dev in zip((1, 3, 2), devs):
            src = (p - off + 4) % 4
            self.sent += [(blk(p, 0), dev, blk(src, 0)), (blk(p, 1), dev, blk(src, 1)), (aux(p), dev, aux(src))]

    def copy(self, k, ref=None):
        ref = self.sent[k][0] if ref is None else ref
        return pltpu.make_async_remote_copy(ref, ref, self.ssem.at[self.row, k], self.rsem.at[self.row, k], device_id=self.sent[k][1], device_id_type=MESH)

    def start_own(self):
        for k in range(9):
            self.copy(k).start()

    def recv_all(self):
        for k in range(9):
            self.copy(k, self.sent[k][2]).wait_recv()

    def wait_sends(self):
        for k in range(9):
            self.copy(k).wait_send()


class Ring:
    def __init__(self, blk, aux, p, right, left, ssem, rsem, row):
        prev, nxt, opp = (p + 3) % 4, (p + 1) % 4, (p + 2) % 4
        self.ssem, self.rsem, self.row = ssem, rsem, row
        self.sent = (
            (blk(p, 0), right, blk(prev, 0)),
            (blk(p, 1), left, blk(nxt, 1)),
            (aux(p), right, aux(prev)),
            (blk(p, 1), right, blk(prev, 1)),
            (blk(p, 0), left, blk(nxt, 0)),
            (aux(p), left, aux(nxt)),
            (blk(prev, 0), right, blk(opp, 0)),
            (blk(nxt, 1), left, blk(opp, 1)),
            (aux(prev), right, aux(opp)),
        )

    def copy(self, k, ref=None):
        ref = self.sent[k][0] if ref is None else ref
        return pltpu.make_async_remote_copy(ref, ref, self.ssem.at[self.row, k], self.rsem.at[self.row, k], device_id=self.sent[k][1], device_id_type=MESH)

    def recv(self, k):
        self.copy(k, self.sent[k][2]).wait_recv()

    def start_own(self):
        for k in range(6):
            self.copy(k).start()

    def forward(self, keys=(0, 1, 2)):
        for k in keys:
            self.recv(k)
            self.copy(k + 6).start()

    def recv_near(self):
        for k in range(3, 6):
            self.recv(k)

    def recv_far(self):
        for k in range(6, 9):
            self.recv(k)

    def wait_sends(self):
        for k in range(9):
            self.copy(k).wait_send()


def kernel(x_h, pos, inv, wdq, wdkv, wkr, gq, gkv, wuq, wqr, wuk, wuv, wout, y_h,
           x_v, wkr_v, wbuf, h0, h1, hkr, tabs, stat, stat_rx, cq, lat, kr, pt,
           uq_v, qr_v, uk_v, uv_v, kcat, vbuf, qt, s_buf, m_s, l_s, acc_s, o_v, og, ysend, ykeep, yrecv, y_v,
           dsem, isem, osem, ssem, rsem, dssem, drsem, psem, assem, arsem, yssem, yrsem, ysem):
    c = lax.axis_index("ctx")
    m = lax.axis_index("model")
    x, y, z = c % 4, (c // 4) % 4, c // 16
    s, d = c // GROUP, c % GROUP
    first = m == 0
    sib = {"ctx": c, "model": 1 - m}
    pa, pb = jnp.where(first, z, y), jnp.where(first, y, z)
    sa, sb = jnp.where(first, 16, 4), jnp.where(first, 4, 16)
    yp = y % 2

    def at(idx):
        return {"ctx": idx, "model": m}

    def near(p, stride):
        return at(c + ((p + 1) % 4 - p) * stride), at(c + ((p + 3) % 4 - p) * stride)

    (xr, xl), (ar, al), (br, bl) = near(x, 1), near(pa, sa), near(pb, sb)
    xo = at(c + (x + 2) % 4 - x)
    ypair = at(c + 4 - 8 * yp)
    peers = [at(c - d + (d + k) % GROUP) for k in range(1, GROUP)]

    def down_copies(k):
        src, dst, slot = pl.ds(2 * k, 2), pl.ds(2 * (k % 4), 2), 2 * (k // 4)
        q0 = pl.multiple_of(m * QH, LANES)
        return (
            pltpu.make_async_copy(wdq.at[src, :, pl.ds(q0, BLK)], wbuf.at[slot, dst], dsem.at[0, k]),
            pltpu.make_async_copy(wdq.at[src, :, pl.ds(pl.multiple_of(q0 + BLK, LANES), QB)], wbuf.at[slot + 1, dst, :, pl.ds(0, QB)], dsem.at[1, k]),
            pltpu.make_async_copy(wdkv.at[src, :, dyn(m, KH)], wbuf.at[slot + 1, dst, :, pl.ds(QB, KH)], dsem.at[2, k]),
        )

    def start_down(k, _):
        for cp in down_copies(k):
            cp.start()
        return 0

    def out_copy(t):
        slot = lax.rem(t, N_SLOTS)
        return pltpu.make_async_copy(wout.at[:, t // N_OUT, :, dyn(lax.rem(t, N_OUT), BLK)], wbuf.at[slot], osem.at[slot])

    ins = [
        pltpu.make_async_copy(a, b, isem.at[i])
        for i, (a, b) in enumerate((
            (x_h, x_v), (wkr, wkr_v), (wuq.at[:, dyn(d, BLK)], uq_v), (wqr.at[:, dyn(d, QB)], qr_v),
            (wuk.at[:, dyn(d, BLK)], uk_v), (wuv.at[:, dyn(d, BLK)], uv_v),
        ))
    ]
    for cp in ins[:2]:
        cp.start()
    lax.fori_loop(0, N_DOWN, start_down, 0)

    sem = pltpu.get_barrier_semaphore()
    greet = peers + [ar, al, br, bl, sib]
    for dev in greet:
        pl.semaphore_signal(sem, inc=1, device_id=dev, device_id_type=MESH)

    ang = inv[...] * pos[...].astype(F32)
    cos_f, sin_f = jnp.cos(ang), jnp.sin(ang)
    tabs[...] = jnp.transpose(jnp.concatenate([cos_f, cos_f, -sin_f, sin_f], axis=0))
    cs = jnp.transpose(jnp.concatenate([cos_f, sin_f], axis=0))

    def pack(v):
        return jnp.concatenate([v[:HALF_SPAN], v[HALF_SPAN:]], axis=-1)

    pt[m, yp, x] = pack(jnp.where(first, cs[:SPAN], cs[SPAN:]))

    h0[...] = jnp.zeros_like(h0)
    h1[...] = jnp.zeros_like(h1)
    hkr[...] = jnp.zeros_like(hkr)
    for cp in ins[:2]:
        cp.wait()

    def down(k, _):
        for cp in down_copies(k):
            cp.wait()
        slot, rows = 2 * (k // 4), pl.ds(2 * (k % 4), 2)
        xb = x_v[:, dyn(k, BLK)]
        h0[...] += dot(xb, wbuf[slot, rows].reshape(BLK, BLK))
        h1[...] += dot(xb, wbuf[slot + 1, rows].reshape(BLK, BLK))
        hkr[...] += dot_dims(xb, wkr_v[:, dyn(k, BLK)], 1, 1)
        return 0

    lax.fori_loop(0, N_DOWN, down, 0)
    for cp in ins[2:]:
        cp.start()
    for j in range(N_SLOTS):
        out_copy(j).start()

    h_q = jnp.concatenate([h0[...], h1[:, :QB]], axis=-1)
    h_kv = h1[:, QB:]
    own_q = jnp.sum(h_q * h_q, axis=-1, keepdims=True)
    own_kv = jnp.sum(h_kv * h_kv, axis=-1, keepdims=True)
    stat[...] = jnp.where(iota((TOK, LANES), 1) < TOK, own_q, own_kv)
    pl.semaphore_wait(sem, len(greet))
    st = pltpu.make_async_remote_copy(stat, stat_rx, psem.at[0], psem.at[1], device_id=sib, device_id_type=MESH)
    st.start()

    k_raw = hkr[...]
    swapped = jnp.concatenate([k_raw[:, SPAN:], k_raw[:, :SPAN]], axis=-1)
    k_rot = k_raw * tabs[:, :TOK] + swapped * tabs[:, TOK:]
    kr[m, pa, pb, x] = pack(jnp.where(first, k_rot[:SPAN], k_rot[SPAN:])).astype(BF)

    st.wait()
    tot_q = own_q + stat_rx[:, :1]
    tot_kv = own_kv + stat_rx[:, TOK:TOK + 1]
    nq, nk = QH // LANES, KH // LANES
    g_q = jnp.concatenate([gq[pl.ds(nq * m + i, 1), :] for i in range(nq)], axis=-1)
    g_kv = jnp.concatenate([gkv[pl.ds(nk * m + i, 1), :] for i in range(nk)], axis=-1)
    c_q = (h_q * lax.rsqrt(tot_q / Q_RANK + NORM_EPS) * g_q).astype(BF)
    c_kv = (h_kv * lax.rsqrt(tot_kv / KV_RANK + NORM_EPS) * g_kv).astype(BF)
    for half in range(2):
        lat[m, half, pa, pb, x] = c_kv[SPAN * half:SPAN * half + SPAN]
        cq[m, half, yp, x] = c_q[SPAN * half:SPAN * half + SPAN]

    def share(ref, k):
        return pltpu.make_async_remote_copy(ref, ref, dssem.at[k], drsem.at[k], device_id=sib, device_id_type=MESH)

    def row_ring(b, row):
        return Ring(lambda p, h: lat.at[m, h, p, b], lambda p: kr.at[m, p, b], pa, ar, al, ssem, rsem, row)

    r1 = Direct(lambda p, h: lat.at[m, h, pa, pb, p], lambda p: kr.at[m, pa, pb, p], x, (xr, xl, xo), ssem, rsem, 0)
    r2 = Ring(lambda p, h: lat.at[m, h, pa, p], lambda p: kr.at[m, pa, p], pb, br, bl, ssem, rsem, 1)
    rq = Ring(lambda p, h: cq.at[m, h, :, p], lambda p: pt.at[m, :, p], x, xr, xl, ssem, rsem, 2)
    r3 = [row_ring((pb + k) % 4, 3 + k) for k in range(4)]
    nxt, prev, opp = (pa + 1) % 4, (pa + 3) % 4, (pa + 2) % 4

    def pair_copies(par):
        return [
            pltpu.make_async_remote_copy(ref, ref, psem.at[2 + i], psem.at[4 + i], device_id=ypair, device_id_type=MESH)
            for i, ref in enumerate((cq.at[m, :, par, x], pt.at[m, par, x]))
        ]

    def shares(core, own, planes, rows):
        refs = [cq.at[core], pt.at[core], lat.at[core, :, own], kr.at[core, own]]
        for b in rows:
            for p in planes:
                refs += [lat.at[core, :, p, b], kr.at[core, p, b]]
        return [share(ref, k) for k, ref in enumerate(refs)]

    mine = shares(m, pa, (prev, nxt, opp), [(pb + k) % 4 for k in range(4)])

    def start_shares(first_k, count):
        for cp in mine[first_k:first_k + count]:
            cp.start()

    def row_near(k):
        r3[k].forward()
        r3[k].recv_near()
        start_shares(4 + 6 * k, 4)

    def row_far(k):
        r3[k].recv_far()
        start_shares(8 + 6 * k, 2)

    r1.start_own()
    for cp in pair_copies(yp):
        cp.start()
    r1.recv_all()
    r2.start_own()
    for cp in pair_copies(1 - yp):
        cp.wait_recv()
    rq.start_own()
    r2.forward((0,))
    r3[0].start_own()
    r2.forward((1, 2))
    r2.recv_near()
    r3[1].start_own()
    r3[3].start_own()
    r2.recv_far()
    r3[2].start_own()
    start_shares(2, 2)
    rq.forward()
    row_near(0)
    row_near(1)
    row_near(3)
    rq.recv_near()
    rq.recv_far()
    start_shares(0, 2)
    row_near(2)
    row_far(0)

    theirs = shares(1 - m, 0, (0, 0, 0), range(4))
    for cp in theirs[:2]:
        cp.wait_recv()
    for cp in ins[2:4]:
        cp.wait()
    t = pt[...].reshape(2 * LANES, LANES)
    grp = iota((2 * LANES, LANES), 1) // SPAN

    def both(shift):
        parts = []
        for extra in (0, TOK):
            v = pltpu.roll(t, (shift + extra) % LANES, 1) if shift + extra else t
            r = v
            for g in range(1, 4):
                r = jnp.where(grp == g, pltpu.roll(v, SPAN * g, 1), r)
            parts.append(r.reshape(HALF_SPAN, HALF_SPAN, LANES))
        return jnp.concatenate(parts, axis=1).reshape(BLK, LANES)

    lower = iota((BLK, LANES), 1) % TOK < SPAN
    cos_t = both(0)
    sin_t = both(LANES - SPAN)
    sin_t = jnp.where(lower, -sin_t, sin_t)
    c0, c1 = cq[0].reshape(BLK, QH), cq[1].reshape(BLK, QH)
    for p in range(2):
        wide, thin = slice(QB * p, QB * p + QB), slice(LANES * p, LANES * p + LANES)
        qn = dot(c0, uq_v[:QH, wide]) + dot(c1, uq_v[QH:, wide])
        qr = dot(c0, qr_v[:QH, thin]) + dot(c1, qr_v[QH:, thin])
        rot = jnp.where(lower, pltpu.roll(qr, LANES - SPAN, 1), pltpu.roll(qr, SPAN, 1))
        qn_t = jnp.transpose(qn).astype(BF)
        qr_t = jnp.transpose(qr * cos_t + rot * sin_t).astype(BF)
        for a in range(2):
            qt[2 * p + a, :LANES, :] = qn_t[LANES * a:LANES * a + LANES]
            qt[2 * p + a, LANES:QK_DIM, :] = qr_t[TOK * a:TOK * a + TOK]
        for k in ((1, 3), (2,))[p]:
            row_far(k)

    for cp in ins[4:]:
        cp.wait()
    for cp in theirs[2:]:
        cp.wait_recv()

    for half in range(2):
        if half == 0:
            k2 = kr[0].reshape(ROWS_H // 2, LANES).astype(F32)
        else:
            k2 = jnp.concatenate([kr[1, :, zz].reshape(QB, LANES) for zz in range(4)], axis=0).astype(F32)
        lo = k2.reshape(TOK, HALF_SPAN, LANES)[:, :, :TOK]
        hi = pltpu.roll(k2, TOK, 1).reshape(TOK, HALF_SPAN, LANES)[:, :, :TOK]
        k3 = jnp.concatenate([lo, hi], axis=1).astype(BF).reshape(ROWS_H, TOK)
        for a in range(2):
            kcat[a, ROWS_H * half:ROWS_H * half + ROWS_H, LANES:QK_DIM] = k3

    nlow = s // 2 + 1

    def place(i):
        low = i < nlow
        b = jnp.where(low, i, i - nlow)
        return low, jnp.where(low, 0, 1), b, jnp.where(b < 4, b, 11 - b)

    def attn_sends(p):
        return [
            pltpu.make_async_remote_copy(
                o_v.at[p, :, (d + k) % GROUP], og.at[p, :, :, dyn(d, QB)],
                assem.at[p, k - 1], arsem.at[p, k - 1], device_id=peers[k - 1], device_id_type=MESH)
            for k in range(1, GROUP)
        ]

    def pair(p, _):
        pc = dyn(p, QB)

        def up(i, _):
            a0 = lat[0, i].reshape(ROWS_H, KH)
            a1 = jnp.concatenate([lat[1, i, :, k].reshape(BLK, KH) for k in range(4)], axis=0)
            rows = pl.ds(pl.multiple_of(i * ROWS_H, BLK), ROWS_H)
            kn = (dot(a0, uk_v[:KH, pc]) + dot(a1, uk_v[KH:, pc])).astype(BF)
            kcat[0, rows, :LANES] = kn[:, :LANES]
            kcat[1, rows, :LANES] = kn[:, LANES:]
            vbuf[rows, :] = (dot(a0, uv_v[:KH, pc]) + dot(a1, uv_v[KH:, pc])).astype(BF)
            return 0

        lax.fori_loop(0, 2, up, 0)
        m_s[...] = jnp.full(m_s.shape, NEG_BIG, F32)
        l_s[...] = jnp.zeros_like(l_s)
        acc_s[...] = jnp.zeros_like(acc_s)

        def scores(i, a):
            _, qb, _, kb = place(i)
            return dot(kcat[a, dyn(kb, BLK), :QK_DIM], qt[2 * p + a, :, dyn(qb, QB)])

        for a in range(2):
            s_buf[a] = scores(0, a)

        def tile(i, _):
            low, qb, b, kb = place(i)

            @pl.when(b == jnp.where(low, s // 2, 7 - s // 2))
            def _():
                r = iota((BLK, 1), 0)
                cc = iota((1, QB), 1)
                k_idx = BLK * b + jnp.where(b < 4, r, (15 - r // SPAN) * SPAN + r % SPAN)
                q_idx = jnp.where(low, QB * s + cc, SPAN * (LANES - 1 - GROUP * s - cc // SPAN) + cc % SPAN)
                allowed = k_idx <= q_idx
                for a in range(2):
                    s_buf[a] = jnp.where(allowed, s_buf[a], NEG_BIG)

            after = jnp.minimum(i + 1, N_TILES - 1)
            for a in range(2):
                sc = s_buf[a]
                m_old = m_s[a, qb, :1, :]
                m_new = jnp.maximum(m_old, jnp.max(sc, axis=0, keepdims=True))
                e = jnp.exp2((sc - m_new) * EXP_SCALE)
                alpha = jnp.exp2((m_old - m_new) * EXP_SCALE)
                l_s[a, qb, :1, :] = l_s[a, qb, :1, :] * alpha + jnp.sum(e, axis=0, keepdims=True)
                s_buf[a] = scores(after, a)
                pv = dot_dims(vbuf[dyn(kb, BLK), LANES * a:LANES * a + LANES], e.astype(BF), 0, 0)
                acc_s[a, qb] = acc_s[a, qb] * alpha + pv
                m_s[a, qb, :1, :] = m_new
            return 0

        lax.fori_loop(0, N_TILES, tile, 0)
        for a in range(2):
            for qb in range(2):
                ot = acc_s[a, qb] / l_s[a, qb, :1, :]
                o_v[p, qb, :, :, LANES * a:LANES * a + LANES] = jnp.transpose(ot).astype(BF).reshape(GROUP, SPAN, LANES)
        for cp in attn_sends(p):
            cp.start()
        og[p, :, :, dyn(d, QB)] = o_v[p, :, d]
        return 0

    lax.fori_loop(0, 2, pair, 0)

    for r in [r1, r2, rq] + r3:
        r.wait_sends()
    for cp in pair_copies(yp) + mine:
        cp.wait_send()
    for cp in attn_sends(0):
        cp.wait()

    def y_copy(j):
        return pltpu.make_async_remote_copy(ysend.at[j], yrecv.at[j], yssem.at[j], yrsem.at[j], device_id=sib, device_id_type=MESH)

    def y_out(j):
        return pltpu.make_async_copy(y_v.at[j], y_h.at[:, dyn(j, BLK)], ysem.at[j])

    def finish(j):
        y_copy(j).wait()
        y_v[j] = (ykeep[j, :SPAN] + yrecv[j]).astype(BF)
        y_out(j).start()

    def half_dot(t):
        out_copy(t).wait()
        return dot(og[t // N_OUT].reshape(TOK, ROWS_H), wbuf[lax.rem(t, N_SLOTS)].reshape(ROWS_H, BLK))

    def refill(t):
        @pl.when(t + N_SLOTS < 2 * N_OUT)
        def _():
            out_copy(t + N_SLOTS).start()

    def first_half(j, _):
        ykeep[j] = half_dot(j)
        refill(j)
        return 0

    lax.fori_loop(0, N_OUT, first_half, 0)
    for cp in attn_sends(1):
        cp.wait()

    def second_half(j, _):
        acc = ykeep[j] + half_dot(j + N_OUT)
        ykeep[j, :SPAN] = jnp.where(first, acc[:SPAN], acc[SPAN:])
        ysend[j] = jnp.where(first, acc[SPAN:], acc[:SPAN])
        y_copy(j).start()
        refill(j + N_OUT)

        @pl.when(j >= LAG)
        def _():
            finish(j - LAG)
        return 0

    lax.fori_loop(0, N_OUT, second_half, 0)
    for j in range(N_OUT - LAG, N_OUT):
        finish(j)

    def drain(j, _):
        y_out(j).wait()
        return 0

    lax.fori_loop(0, N_OUT, drain, 0)


def fused(x, pos, inv, wdq, wdkv, wkr, gq, gkv, wuq, wqr, wuk, wuv, wout):
    vm = pl.BlockSpec(memory_space=pltpu.VMEM)
    hbm = pl.BlockSpec(memory_space=pl.ANY)
    v, dma = pltpu.VMEM, pltpu.SemaphoreType.DMA
    state = v((2, 2, 8, QB), F32)
    part = v((N_OUT, SPAN, BLK), F32)
    return pl.pallas_call(
        kernel,
        name="mla_prefill",
        out_shape=jax.ShapeDtypeStruct((SPAN, HIDDEN), BF),
        in_specs=[hbm, vm, vm, hbm, hbm, hbm, vm, vm] + [hbm] * 5,
        out_specs=hbm,
        scratch_shapes=[
            v((TOK, HIDDEN), BF), v((TOK, HIDDEN), BF), v((N_SLOTS, GROUP, QB, BLK), BF),
            v((TOK, BLK), F32), v((TOK, BLK), F32), v((TOK, TOK), F32), v((TOK, LANES), F32), v((TOK, LANES), F32), v((TOK, LANES), F32),
            v((2, 2, 2, 4, SPAN, QH), BF), v((2, 2, 4, 4, 4, SPAN, KH), BF), v((2, 4, 4, 4, HALF_SPAN, LANES), BF), v((2, 2, 4, HALF_SPAN, LANES), F32),
            v((Q_RANK, BLK), BF), v((Q_RANK, QB), BF), v((KV_RANK, BLK), BF), v((KV_RANK, BLK), BF),
            v((2, KEYS, QB), BF), v((KEYS, QB), BF), v((4, QK_DIM, BLK), BF), v((2, BLK, QB), F32),
            state, state, v((2, 2, LANES, QB), F32), v((2, 2, GROUP, SPAN, QB), BF), v((2, 2, SPAN, ROWS_H), BF), part, v((N_OUT, TOK, BLK), F32), part, v((N_OUT, SPAN, BLK), BF),
            dma((3, N_DOWN)), dma((6,)), dma((N_SLOTS,)), dma((7, 9)), dma((7, 9)), dma((28,)), dma((28,)), dma((6,)),
            dma((2, 7)), dma((2, 7)), dma((N_OUT,)), dma((N_OUT,)), dma((N_OUT,)),
        ],
        compiler_params=pltpu.CompilerParams(collective_id=0, has_side_effects=True, vmem_limit_bytes=LIMIT),
    )(x, pos, inv, wdq, wdkv, wkr, gq, gkv, wuq, wqr, wuk, wuv, wout)


def solution(mesh):
    freq = ROPE_BASE ** (-np.arange(SPAN) * 2.0 / TOK)
    inv = np.repeat(freq.astype(np.float32)[:, None], TOK, axis=1)

    def local(x_tokens, positions, w_dq, gain_q, w_uq, w_qr, w_dkv, gain_kv, w_kr, w_uk, w_uv, w_out):
        return fused(x_tokens, positions[None], inv, w_dq.reshape(-1, QB, Q_RANK), w_dkv.reshape(-1, QB, KV_RANK), w_kr.T, gain_q.reshape(-1, LANES), gain_kv.reshape(-1, LANES), w_uq, w_qr, w_uk, w_uv, w_out.reshape(GROUP, 2, QB, HIDDEN))

    in_specs = (P(('dp', 'ctx'), None), P(('dp', 'ctx')), P(), P(), P(None, 'model'), P(None, 'model'), P(), P(), P(), P(None, 'model'), P(None, 'model'), P('model', None))
    out_specs = P(('dp', 'ctx', 'model'), None)
    return jax.shard_map(local, mesh=mesh, in_specs=in_specs, out_specs=out_specs, check_vma=False)
```

```python
import math

import numpy as np
import jax
import jax.numpy as jnp
from jax import lax
from jax.experimental import pallas as pl
from jax.experimental.pallas import tpu as pltpu
from jax.sharding import PartitionSpec as P

NORM_EPS = 1e-6
ROPE_BASE = 10000.0
NEG_BIG = -1e30
MESH = pl.DeviceIdType.MESH
BF = jnp.bfloat16
F32 = jnp.float32

HIDDEN = 7168
Q_RANK = 1536
KV_RANK = 512
TOK = 64
SPAN = 32
HALF_SPAN = SPAN // 2
LANES = 128
QH = Q_RANK // 2
KH = KV_RANK // 2
BLK = 512
QB = 256
QK_DIM = 192
KEYS = 4096
ROWS_H = KEYS // 2
N_DOWN = HIDDEN // BLK
N_OUT = HIDDEN // BLK
N_SLOTS = 16
LAG = 3
N_TILES = 9
GROUP = 8
EXP_SCALE = QK_DIM ** -0.5 * math.log2(math.e)
LIMIT = 66 * 10 ** 6


def dot(a, b):
    return jnp.dot(a, b, preferred_element_type=F32)


def dot_dims(a, b, ca, cb):
    return lax.dot_general(a, b, (((ca,), (cb,)), ((), ())), preferred_element_type=F32)


def iota(shape, axis):
    return lax.broadcasted_iota(jnp.int32, shape, axis)


def dyn(i, width):
    return pl.ds(pl.multiple_of(i * width, math.gcd(width, BLK)), width)


class Direct:
    def __init__(self, blk, aux, p, devs, ssem, rsem, row):
        self.ssem, self.rsem, self.row = ssem, rsem, row
        self.sent = []
        for off, dev in zip((1, 3, 2), devs):
            src = (p - off + 4) % 4
            self.sent += [(blk(p, 0), dev, blk(src, 0)), (blk(p, 1), dev, blk(src, 1)), (aux(p), dev, aux(src))]

    def copy(self, k, ref=None):
        ref = self.sent[k][0] if ref is None else ref
        return pltpu.make_async_remote_copy(ref, ref, self.ssem.at[self.row, k], self.rsem.at[self.row, k], device_id=self.sent[k][1], device_id_type=MESH)

    def start_own(self):
        for k in range(9):
            self.copy(k).start()

    def recv_all(self):
        for k in range(9):
            self.copy(k, self.sent[k][2]).wait_recv()

    def wait_sends(self):
        for k in range(9):
            self.copy(k).wait_send()


class Ring:
    def __init__(self, blk, aux, p, right, left, ssem, rsem, row):
        prev, nxt, opp = (p + 3) % 4, (p + 1) % 4, (p + 2) % 4
        self.ssem, self.rsem, self.row = ssem, rsem, row
        self.sent = (
            (blk(p, 0), right, blk(prev, 0)),
            (blk(p, 1), left, blk(nxt, 1)),
            (aux(p), right, aux(prev)),
            (blk(p, 1), right, blk(prev, 1)),
            (blk(p, 0), left, blk(nxt, 0)),
            (aux(p), left, aux(nxt)),
            (blk(prev, 0), right, blk(opp, 0)),
            (blk(nxt, 1), left, blk(opp, 1)),
            (aux(prev), right, aux(opp)),
        )

    def copy(self, k, ref=None):
        ref = self.sent[k][0] if ref is None else ref
        return pltpu.make_async_remote_copy(ref, ref, self.ssem.at[self.row, k], self.rsem.at[self.row, k], device_id=self.sent[k][1], device_id_type=MESH)

    def recv(self, k):
        self.copy(k, self.sent[k][2]).wait_recv()

    def start_own(self):
        for k in range(6):
            self.copy(k).start()

    def forward(self, keys=(0, 1, 2)):
        for k in keys:
            self.recv(k)
            self.copy(k + 6).start()

    def recv_near(self):
        for k in range(3, 6):
            self.recv(k)

    def recv_far(self):
        for k in range(6, 9):
            self.recv(k)

    def wait_sends(self):
        for k in range(9):
            self.copy(k).wait_send()


def kernel(x_h, pos, inv, wdq, wdkv, wkr, gq, gkv, wuq, wqr, wuk, wuv, wout, y_h,
           x_v, wkr_v, wbuf, h0, h1, hkr, tabs, stat, stat_rx, cq, lat, kr, pt,
           uq_v, qr_v, uk_v, uv_v, kcat, vbuf, qt, s_buf, m_s, l_s, acc_s, o_v, og, ysend, ykeep, yrecv, y_v,
           dsem, isem, osem, ssem, rsem, dssem, drsem, psem, assem, arsem, yssem, yrsem, ysem):
    c = lax.axis_index("ctx")
    m = lax.axis_index("model")
    x, y, z = c % 4, (c // 4) % 4, c // 16
    s, d = c // GROUP, c % GROUP
    first = m == 0
    sib = {"ctx": c, "model": 1 - m}
    pa, pb = jnp.where(first, z, y), jnp.where(first, y, z)
    sa, sb = jnp.where(first, 16, 4), jnp.where(first, 4, 16)
    yp = y % 2

    def at(idx):
        return {"ctx": idx, "model": m}

    def near(p, stride):
        return at(c + ((p + 1) % 4 - p) * stride), at(c + ((p + 3) % 4 - p) * stride)

    (xr, xl), (ar, al), (br, bl) = near(x, 1), near(pa, sa), near(pb, sb)
    xo = at(c + (x + 2) % 4 - x)
    ypair = at(c + 4 - 8 * yp)
    peers = [at(c - d + (d + k) % GROUP) for k in range(1, GROUP)]

    def down_copies(k):
        src, dst, slot = pl.ds(2 * k, 2), pl.ds(2 * (k % 4), 2), 2 * (k // 4)
        q0 = pl.multiple_of(m * QH, LANES)
        return (
            pltpu.make_async_copy(wdq.at[src, :, pl.ds(q0, BLK)], wbuf.at[slot, dst], dsem.at[0, k]),
            pltpu.make_async_copy(wdq.at[src, :, pl.ds(pl.multiple_of(q0 + BLK, LANES), QB)], wbuf.at[slot + 1, dst, :, pl.ds(0, QB)], dsem.at[1, k]),
            pltpu.make_async_copy(wdkv.at[src, :, dyn(m, KH)], wbuf.at[slot + 1, dst, :, pl.ds(QB, KH)], dsem.at[2, k]),
        )

    def start_down(k, _):
        for cp in down_copies(k):
            cp.start()
        return 0

    def out_copy(t):
        slot = lax.rem(t, N_SLOTS)
        return pltpu.make_async_copy(wout.at[:, t // N_OUT, :, dyn(lax.rem(t, N_OUT), BLK)], wbuf.at[slot], osem.at[slot])

    ins = [
        pltpu.make_async_copy(a, b, isem.at[i])
        for i, (a, b) in enumerate((
            (x_h, x_v), (wkr, wkr_v), (wuq.at[:, dyn(d, BLK)], uq_v), (wqr.at[:, dyn(d, QB)], qr_v),
            (wuk.at[:, dyn(d, BLK)], uk_v), (wuv.at[:, dyn(d, BLK)], uv_v),
        ))
    ]
    for cp in ins[:2]:
        cp.start()
    lax.fori_loop(0, N_DOWN, start_down, 0)

    sem = pltpu.get_barrier_semaphore()
    greet = peers + [ar, al, br, bl, sib]
    for dev in greet:
        pl.semaphore_signal(sem, inc=1, device_id=dev, device_id_type=MESH)

    ang = inv[...] * pos[...].astype(F32)
    cos_f, sin_f = jnp.cos(ang), jnp.sin(ang)
    tabs[...] = jnp.transpose(jnp.concatenate([cos_f, cos_f, -sin_f, sin_f], axis=0))
    cs = jnp.transpose(jnp.concatenate([cos_f, sin_f], axis=0))

    def pack(v):
        return jnp.concatenate([v[:HALF_SPAN], v[HALF_SPAN:]], axis=-1)

    pt[m, yp, x] = pack(jnp.where(first, cs[:SPAN], cs[SPAN:]))

    h0[...] = jnp.zeros_like(h0)
    h1[...] = jnp.zeros_like(h1)
    hkr[...] = jnp.zeros_like(hkr)
    for cp in ins[:2]:
        cp.wait()

    def down(k, _):
        for cp in down_copies(k):
            cp.wait()
        slot, rows = 2 * (k // 4), pl.ds(2 * (k % 4), 2)
        xb = x_v[:, dyn(k, BLK)]
        h0[...] += dot(xb, wbuf[slot, rows].reshape(BLK, BLK))
        h1[...] += dot(xb, wbuf[slot + 1, rows].reshape(BLK, BLK))
        hkr[...] += dot_dims(xb, wkr_v[:, dyn(k, BLK)], 1, 1)
        return 0

    lax.fori_loop(0, N_DOWN, down, 0)
    for cp in ins[2:]:
        cp.start()
    for j in range(N_SLOTS):
        out_copy(j).start()

    h_q = jnp.concatenate([h0[...], h1[:, :QB]], axis=-1)
    h_kv = h1[:, QB:]
    own_q = jnp.sum(h_q * h_q, axis=-1, keepdims=True)
    own_kv = jnp.sum(h_kv * h_kv, axis=-1, keepdims=True)
    stat[...] = jnp.where(iota((TOK, LANES), 1) < TOK, own_q, own_kv)
    pl.semaphore_wait(sem, len(greet))
    st = pltpu.make_async_remote_copy(stat, stat_rx, psem.at[0], psem.at[1], device_id=sib, device_id_type=MESH)
    st.start()

    k_raw = hkr[...]
    swapped = jnp.concatenate([k_raw[:, SPAN:], k_raw[:, :SPAN]], axis=-1)
    k_rot = k_raw * tabs[:, :TOK] + swapped * tabs[:, TOK:]
    kr[m, pa, pb, x] = pack(jnp.where(first, k_rot[:SPAN], k_rot[SPAN:])).astype(BF)

    st.wait()
    tot_q = own_q + stat_rx[:, :1]
    tot_kv = own_kv + stat_rx[:, TOK:TOK + 1]
    nq, nk = QH // LANES, KH // LANES
    g_q = jnp.concatenate([gq[pl.ds(nq * m + i, 1), :] for i in range(nq)], axis=-1)
    g_kv = jnp.concatenate([gkv[pl.ds(nk * m + i, 1), :] for i in range(nk)], axis=-1)
    c_q = (h_q * lax.rsqrt(tot_q / Q_RANK + NORM_EPS) * g_q).astype(BF)
    c_kv = (h_kv * lax.rsqrt(tot_kv / KV_RANK + NORM_EPS) * g_kv).astype(BF)
    for half in range(2):
        lat[m, half, pa, pb, x] = c_kv[SPAN * half:SPAN * half + SPAN]
        cq[m, half, yp, x] = c_q[SPAN * half:SPAN * half + SPAN]

    def share(ref, k):
        return pltpu.make_async_remote_copy(ref, ref, dssem.at[k], drsem.at[k], device_id=sib, device_id_type=MESH)

    def row_ring(b, row):
        return Ring(lambda p, h: lat.at[m, h, p, b], lambda p: kr.at[m, p, b], pa, ar, al, ssem, rsem, row)

    r1 = Direct(lambda p, h: lat.at[m, h, pa, pb, p], lambda p: kr.at[m, pa, pb, p], x, (xr, xl, xo), ssem, rsem, 0)
    r2 = Ring(lambda p, h: lat.at[m, h, pa, p], lambda p: kr.at[m, pa, p], pb, br, bl, ssem, rsem, 1)
    rq = Ring(lambda p, h: cq.at[m, h, :, p], lambda p: pt.at[m, :, p], x, xr, xl, ssem, rsem, 2)
    r3 = [row_ring((pb + k) % 4, 3 + k) for k in range(4)]
    nxt, prev, opp = (pa + 1) % 4, (pa + 3) % 4, (pa + 2) % 4

    def pair_copies(par):
        return [
            pltpu.make_async_remote_copy(ref, ref, psem.at[2 + i], psem.at[4 + i], device_id=ypair, device_id_type=MESH)
            for i, ref in enumerate((cq.at[m, :, par, x], pt.at[m, par, x]))
        ]

    def shares(core, own, planes, rows):
        refs = [cq.at[core], pt.at[core], lat.at[core, :, own], kr.at[core, own]]
        for b in rows:
            for p in planes:
                refs += [lat.at[core, :, p, b], kr.at[core, p, b]]
        return [share(ref, k) for k, ref in enumerate(refs)]

    mine = shares(m, pa, (prev, nxt, opp), [(pb + k) % 4 for k in range(4)])

    def start_shares(first_k, count):
        for cp in mine[first_k:first_k + count]:
            cp.start()

    def row_near(k):
        r3[k].forward()
        r3[k].recv_near()
        start_shares(4 + 6 * k, 4)

    def row_far(k):
        r3[k].recv_far()
        start_shares(8 + 6 * k, 2)

    r1.start_own()
    for cp in pair_copies(yp):
        cp.start()
    r1.recv_all()
    r2.start_own()
    for cp in pair_copies(1 - yp):
        cp.wait_recv()
    rq.start_own()
    r2.forward((0,))
    r3[0].start_own()
    r2.forward((1, 2))
    r2.recv_near()
    r3[1].start_own()
    r3[3].start_own()
    r2.recv_far()
    r3[2].start_own()
    start_shares(2, 2)
    rq.forward()
    row_near(0)
    rq.recv_near()
    rq.recv_far()
    start_shares(0, 2)
    row_near(1)
    row_near(3)

    theirs = shares(1 - m, 0, (0, 0, 0), range(4))
    for cp in theirs[:2]:
        cp.wait_recv()
    for cp in ins[2:4]:
        cp.wait()
    t = pt[...].reshape(2 * LANES, LANES)
    grp = iota((2 * LANES, LANES), 1) // SPAN

    def both(shift):
        parts = []
        for extra in (0, TOK):
            v = pltpu.roll(t, (shift + extra) % LANES, 1) if shift + extra else t
            r = v
            for g in range(1, 4):
                r = jnp.where(grp == g, pltpu.roll(v, SPAN * g, 1), r)
            parts.append(r.reshape(HALF_SPAN, HALF_SPAN, LANES))
        return jnp.concatenate(parts, axis=1).reshape(BLK, LANES)

    lower = iota((BLK, LANES), 1) % TOK < SPAN
    cos_t = both(0)
    sin_t = both(LANES - SPAN)
    sin_t = jnp.where(lower, -sin_t, sin_t)

    def queries(p):
        c0, c1 = cq[0].reshape(BLK, QH), cq[1].reshape(BLK, QH)
        wide, thin = slice(QB * p, QB * p + QB), slice(LANES * p, LANES * p + LANES)
        qn = dot(c0, uq_v[:QH, wide]) + dot(c1, uq_v[QH:, wide])
        qr = dot(c0, qr_v[:QH, thin]) + dot(c1, qr_v[QH:, thin])
        rot = jnp.where(lower, pltpu.roll(qr, LANES - SPAN, 1), pltpu.roll(qr, SPAN, 1))
        qn_t = jnp.transpose(qn).astype(BF)
        qr_t = jnp.transpose(qr * cos_t + rot * sin_t).astype(BF)
        for a in range(2):
            qt[2 * p + a, :LANES, :] = qn_t[LANES * a:LANES * a + LANES]
            qt[2 * p + a, LANES:QK_DIM, :] = qr_t[TOK * a:TOK * a + TOK]

    queries(0)
    row_near(2)
    for k in (0, 1, 3):
        row_far(k)
    queries(1)
    row_far(2)

    for cp in ins[4:]:
        cp.wait()
    for cp in theirs[2:]:
        cp.wait_recv()

    for half in range(2):
        if half == 0:
            k2 = kr[0].reshape(ROWS_H // 2, LANES).astype(F32)
        else:
            k2 = jnp.concatenate([kr[1, :, zz].reshape(QB, LANES) for zz in range(4)], axis=0).astype(F32)
        lo = k2.reshape(TOK, HALF_SPAN, LANES)[:, :, :TOK]
        hi = pltpu.roll(k2, TOK, 1).reshape(TOK, HALF_SPAN, LANES)[:, :, :TOK]
        k3 = jnp.concatenate([lo, hi], axis=1).astype(BF).reshape(ROWS_H, TOK)
        for a in range(2):
            kcat[a, ROWS_H * half:ROWS_H * half + ROWS_H, LANES:QK_DIM] = k3

    nlow = s // 2 + 1

    def place(i):
        low = i < nlow
        b = jnp.where(low, i, i - nlow)
        return low, jnp.where(low, 0, 1), b, jnp.where(b < 4, b, 11 - b)

    def attn_sends(p):
        return [
            pltpu.make_async_remote_copy(
                o_v.at[p, :, (d + k) % GROUP], og.at[p, :, :, dyn(d, QB)],
                assem.at[p, k - 1], arsem.at[p, k - 1], device_id=peers[k - 1], device_id_type=MESH)
            for k in range(1, GROUP)
        ]

    def pair(p, _):
        pc = dyn(p, QB)

        def up(i, _):
            a0 = lat[0, i].reshape(ROWS_H, KH)
            a1 = jnp.concatenate([lat[1, i, :, k].reshape(BLK, KH) for k in range(4)], axis=0)
            rows = pl.ds(pl.multiple_of(i * ROWS_H, BLK), ROWS_H)
            kn = (dot(a0, uk_v[:KH, pc]) + dot(a1, uk_v[KH:, pc])).astype(BF)
            kcat[0, rows, :LANES] = kn[:, :LANES]
            kcat[1, rows, :LANES] = kn[:, LANES:]
            vbuf[rows, :] = (dot(a0, uv_v[:KH, pc]) + dot(a1, uv_v[KH:, pc])).astype(BF)
            return 0

        lax.fori_loop(0, 2, up, 0)
        m_s[...] = jnp.full(m_s.shape, NEG_BIG, F32)
        l_s[...] = jnp.zeros_like(l_s)
        acc_s[...] = jnp.zeros_like(acc_s)

        def scores(i, a):
            _, qb, _, kb = place(i)
            return dot(kcat[a, dyn(kb, BLK), :QK_DIM], qt[2 * p + a, :, dyn(qb, QB)])

        for a in range(2):
            s_buf[a] = scores(0, a)

        def tile(i, _):
            low, qb, b, kb = place(i)

            @pl.when(b == jnp.where(low, s // 2, 7 - s // 2))
            def _():
                r = iota((BLK, 1), 0)
                cc = iota((1, QB), 1)
                k_idx = BLK * b + jnp.where(b < 4, r, (15 - r // SPAN) * SPAN + r % SPAN)
                q_idx = jnp.where(low, QB * s + cc, SPAN * (LANES - 1 - GROUP * s - cc // SPAN) + cc % SPAN)
                allowed = k_idx <= q_idx
                for a in range(2):
                    s_buf[a] = jnp.where(allowed, s_buf[a], NEG_BIG)

            after = jnp.minimum(i + 1, N_TILES - 1)
            for a in range(2):
                sc = s_buf[a]
                m_old = m_s[a, qb, :1, :]
                m_new = jnp.maximum(m_old, jnp.max(sc, axis=0, keepdims=True))
                e = jnp.exp2((sc - m_new) * EXP_SCALE)
                alpha = jnp.exp2((m_old - m_new) * EXP_SCALE)
                l_s[a, qb, :1, :] = l_s[a, qb, :1, :] * alpha + jnp.sum(e, axis=0, keepdims=True)
                s_buf[a] = scores(after, a)
                pv = dot_dims(vbuf[dyn(kb, BLK), LANES * a:LANES * a + LANES], e.astype(BF), 0, 0)
                acc_s[a, qb] = acc_s[a, qb] * alpha + pv
                m_s[a, qb, :1, :] = m_new
            return 0

        lax.fori_loop(0, N_TILES, tile, 0)
        for a in range(2):
            for qb in range(2):
                ot = acc_s[a, qb] / l_s[a, qb, :1, :]
                o_v[p, qb, :, :, LANES * a:LANES * a + LANES] = jnp.transpose(ot).astype(BF).reshape(GROUP, SPAN, LANES)
        for cp in attn_sends(p):
            cp.start()
        og[p, :, :, dyn(d, QB)] = o_v[p, :, d]
        return 0

    lax.fori_loop(0, 2, pair, 0)

    for r in [r1, r2, rq] + r3:
        r.wait_sends()
    for cp in pair_copies(yp) + mine:
        cp.wait_send()
    for cp in attn_sends(0):
        cp.wait()

    def y_copy(j):
        return pltpu.make_async_remote_copy(ysend.at[j], yrecv.at[j], yssem.at[j], yrsem.at[j], device_id=sib, device_id_type=MESH)

    def y_out(j):
        return pltpu.make_async_copy(y_v.at[j], y_h.at[:, dyn(j, BLK)], ysem.at[j])

    def finish(j):
        y_copy(j).wait()
        y_v[j] = (ykeep[j, :SPAN] + yrecv[j]).astype(BF)
        y_out(j).start()

    def half_dot(t):
        out_copy(t).wait()
        return dot(og[t // N_OUT].reshape(TOK, ROWS_H), wbuf[lax.rem(t, N_SLOTS)].reshape(ROWS_H, BLK))

    def refill(t):
        @pl.when(t + N_SLOTS < 2 * N_OUT)
        def _():
            out_copy(t + N_SLOTS).start()

    def first_half(j, _):
        ykeep[j] = half_dot(j)
        refill(j)
        return 0

    lax.fori_loop(0, N_OUT, first_half, 0)
    for cp in attn_sends(1):
        cp.wait()

    def second_half(j, _):
        acc = ykeep[j] + half_dot(j + N_OUT)
        ykeep[j, :SPAN] = jnp.where(first, acc[:SPAN], acc[SPAN:])
        ysend[j] = jnp.where(first, acc[SPAN:], acc[:SPAN])
        y_copy(j).start()
        refill(j + N_OUT)

        @pl.when(j >= LAG)
        def _():
            finish(j - LAG)
        return 0

    lax.fori_loop(0, N_OUT, second_half, 0)
    for j in range(N_OUT - LAG, N_OUT):
        finish(j)

    def drain(j, _):
        y_out(j).wait()
        return 0

    lax.fori_loop(0, N_OUT, drain, 0)


def fused(x, pos, inv, wdq, wdkv, wkr, gq, gkv, wuq, wqr, wuk, wuv, wout):
    vm = pl.BlockSpec(memory_space=pltpu.VMEM)
    hbm = pl.BlockSpec(memory_space=pl.ANY)
    v, dma = pltpu.VMEM, pltpu.SemaphoreType.DMA
    state = v((2, 2, 8, QB), F32)
    part = v((N_OUT, SPAN, BLK), F32)
    return pl.pallas_call(
        kernel,
        name="mla_prefill",
        out_shape=jax.ShapeDtypeStruct((SPAN, HIDDEN), BF),
        in_specs=[hbm, vm, vm, hbm, hbm, hbm, vm, vm] + [hbm] * 5,
        out_specs=hbm,
        scratch_shapes=[
            v((TOK, HIDDEN), BF), v((TOK, HIDDEN), BF), v((N_SLOTS, GROUP, QB, BLK), BF),
            v((TOK, BLK), F32), v((TOK, BLK), F32), v((TOK, TOK), F32), v((TOK, LANES), F32), v((TOK, LANES), F32), v((TOK, LANES), F32),
            v((2, 2, 2, 4, SPAN, QH), BF), v((2, 2, 4, 4, 4, SPAN, KH), BF), v((2, 4, 4, 4, HALF_SPAN, LANES), BF), v((2, 2, 4, HALF_SPAN, LANES), F32),
            v((Q_RANK, BLK), BF), v((Q_RANK, QB), BF), v((KV_RANK, BLK), BF), v((KV_RANK, BLK), BF),
            v((2, KEYS, QB), BF), v((KEYS, QB), BF), v((4, QK_DIM, BLK), BF), v((2, BLK, QB), F32),
            state, state, v((2, 2, LANES, QB), F32), v((2, 2, GROUP, SPAN, QB), BF), v((2, 2, SPAN, ROWS_H), BF), part, v((N_OUT, TOK, BLK), F32), part, v((N_OUT, SPAN, BLK), BF),
            dma((3, N_DOWN)), dma((6,)), dma((N_SLOTS,)), dma((7, 9)), dma((7, 9)), dma((28,)), dma((28,)), dma((6,)),
            dma((2, 7)), dma((2, 7)), dma((N_OUT,)), dma((N_OUT,)), dma((N_OUT,)),
        ],
        compiler_params=pltpu.CompilerParams(collective_id=0, has_side_effects=True, vmem_limit_bytes=LIMIT),
    )(x, pos, inv, wdq, wdkv, wkr, gq, gkv, wuq, wqr, wuk, wuv, wout)


def solution(mesh):
    freq = ROPE_BASE ** (-np.arange(SPAN) * 2.0 / TOK)
    inv = np.repeat(freq.astype(np.float32)[:, None], TOK, axis=1)

    def local(x_tokens, positions, w_dq, gain_q, w_uq, w_qr, w_dkv, gain_kv, w_kr, w_uk, w_uv, w_out):
        return fused(x_tokens, positions[None], inv, w_dq.reshape(-1, QB, Q_RANK), w_dkv.reshape(-1, QB, KV_RANK), w_kr.T, gain_q.reshape(-1, LANES), gain_kv.reshape(-1, LANES), w_uq, w_qr, w_uk, w_uv, w_out.reshape(GROUP, 2, QB, HIDDEN))

    in_specs = (P(('dp', 'ctx'), None), P(('dp', 'ctx')), P(), P(), P(None, 'model'), P(None, 'model'), P(), P(), P(), P(None, 'model'), P(None, 'model'), P('model', None))
    out_specs = P(('dp', 'ctx', 'model'), None)
    return jax.shard_map(local, mesh=mesh, in_specs=in_specs, out_specs=out_specs, check_vma=False)
```
